512 devices in a mesh: gx: 8 (over z_lo, core), yz: 64 (over z_hi, y, x).
Axes of the slice: x: 4, y: 8, z: 8 (z_hi: 2, z_lo: 4; z = z_hi * 4 + z_lo), core: 2. Of those that a mesh axis runs over, the one named last changes fastest.
Arguments:
- features_in: bfloat16 [64, 32, 96, 144], P('yz', None, 'gx'), may hold values from -6 to 6
- encode_fine_first: bfloat16 [32, 864], replicated, may hold values from -0.3125 to 0.3125
- encode_fine_second: bfloat16 [32, 864], replicated, may hold values from -0.3125 to 0.3125
- reduce_fine: bfloat16 [64, 256], replicated, may hold values from -0.5 to 0.5
- encode_middle_first: bfloat16 [64, 1728], replicated, may hold values from -0.21875 to 0.21875
- encode_middle_second: bfloat16 [64, 1728], replicated, may hold values from -0.21875 to 0.21875
- reduce_middle: bfloat16 [256, 512], replicated, may hold values from -0.375 to 0.375
- bottom_first: bfloat16 [1024, 1728], P('yz'), may hold values from -0.109375 to 0.109375
- bottom_second: bfloat16 [1024, 1728], P('yz'), may hold values from -0.109375 to 0.109375
- expand_middle: bfloat16 [256, 512], replicated, may hold values from -0.5 to 0.5
- decode_middle_first: bfloat16 [64, 1728], replicated, may hold values from -0.21875 to 0.21875
- decode_middle_second: bfloat16 [64, 1728], replicated, may hold values from -0.21875 to 0.21875
- expand_fine: bfloat16 [64, 256], replicated, may hold values from -1 to 1
- decode_fine_first: bfloat16 [32, 864], replicated, may hold values from -0.3125 to 0.3125
- decode_fine_second: bfloat16 [32, 864], replicated, may hold values from -0.3125 to 0.3125
Outputs:
- features_out: bfloat16 [64, 32, 96, 144], P('yz', None, 'gx')
The draws below stay inside these ranges and needn't reach their ends.
All inputs are finite; a program needn't handle non-finite values.
Results may differ from the reference program's by a relative error of at most 0.023.
Values may be sent and summed in bfloat16 or wider, within the bound.
A program may use at most 128 MiB of HBM per device.

```python
import math
import jax
import jax.numpy as jnp
from jax import lax

C0 = 12
CH0 = 32
CH1 = 64
CB = 256
NX = 96
N_YZ = 64


def level_of(key, shape, split, low, high):
    level, own = 1.0, jax.random.fold_in(key, 6)
    for dim, shards_of in split:
        heights = jnp.exp(jax.random.uniform(jax.random.fold_in(own, dim), (shards_of,), jnp.float32, low / len(split), high / len(split)))
        level = level * jnp.repeat(heights, shape[dim] // shards_of).reshape([-1 if axis == dim else 1 for axis in range(len(shape))])
    return level


def gaussian(rng, shape, scale, limit, pieces=(), kind=jnp.bfloat16):
    array = scale * jax.random.normal(rng, shape, jnp.float32)
    if pieces:
        array = array * level_of(rng, shape, pieces, -0.22, 0.18)
    return jnp.clip(array, -limit, limit).astype(kind)


def setup_inputs(seed: int = 0) -> dict:
    splits = jax.random.split(jax.random.key(seed), 16)
    features_in = gaussian(splits[0], (N_YZ, CH0, NX, C0 * C0), 1.0, 6.0, ((0, 64), (2, 8)))
    encode_fine_first = gaussian(splits[1], (CH0, CH0 * 27), (CH0 * 27 // 2) ** -0.5, 0.3125)
    encode_fine_second = gaussian(splits[2], (CH0, CH0 * 27), (CH0 * 27 // 2) ** -0.5, 0.3125)
    reduce_fine = gaussian(splits[3], (CH1, CH0 * 8), (CH0 * 4) ** -0.5, 0.5)
    encode_middle_first = gaussian(splits[4], (CH1, CH1 * 27), (CH1 * 27 // 2) ** -0.5, 0.21875)
    encode_middle_second = gaussian(splits[5], (CH1, CH1 * 27), (CH1 * 27 // 2) ** -0.5, 0.21875)
    reduce_middle = gaussian(splits[6], (CB, CH1 * 8), (CH1 * 4) ** -0.5, 0.375)
    bottom_first = gaussian(splits[7], (4 * CB, CB * 27 // 4), (CB * 27 // 2) ** -0.5, 0.109375, ((0, 64),))
    bottom_second = gaussian(splits[8], (4 * CB, CB * 27 // 4), (CB * 27 // 2) ** -0.5, 0.109375, ((0, 64),))
    expand_middle = gaussian(splits[9], (CB, CH1 * 8), (CB // 2) ** -0.5, 0.5)
    decode_middle_first = gaussian(splits[10], (CH1, CH1 * 27), (CH1 * 27 // 2) ** -0.5, 0.21875)
    decode_middle_second = gaussian(splits[11], (CH1, CH1 * 27), (CH1 * 27 // 2) ** -0.5, 0.21875)
    expand_fine = gaussian(splits[12], (CH1, CH0 * 8), (CH1 // 2) ** -0.5, 1.0)
    decode_fine_first = gaussian(splits[13], (CH0, CH0 * 27), (CH0 * 27 // 2) ** -0.5, 0.3125)
    decode_fine_second = gaussian(splits[14], (CH0, CH0 * 27), (CH0 * 27 // 2) ** -0.5, 0.3125)
    return {"features_in": features_in, "encode_fine_first": encode_fine_first, "encode_fine_second": encode_fine_second, "reduce_fine": reduce_fine, "encode_middle_first": encode_middle_first, "encode_middle_second": encode_middle_second, "reduce_middle": reduce_middle, "bottom_first": bottom_first, "bottom_second": bottom_second, "expand_middle": expand_middle, "decode_middle_first": decode_middle_first, "decode_middle_second": decode_middle_second, "expand_fine": expand_fine, "decode_fine_first": decode_fine_first, "decode_fine_second": decode_fine_second}


def to_volume(packed, across):
    count, width, extent_x, flat = packed.shape
    extent = math.isqrt(flat)
    shaped = packed.reshape(across, across, width, extent_x, extent, extent)
    return shaped.transpose(2, 3, 0, 4, 1, 5).reshape(width, extent_x, across * extent, across * extent)

def from_volume(volume, across):
    width, extent_x, extent_y, extent_z = volume.shape
    extent = extent_y // across
    shaped = volume.reshape(width, extent_x, across, extent, across, extent)
    return shaped.transpose(2, 4, 0, 1, 3, 5).reshape(across * across, width, extent_x, extent * extent)

def conv_taps(padded, weight, width_in):
    kernel = weight.reshape(weight.shape[0], width_in, 3, 3, 3)
    return lax.conv_general_dilated(padded[None], kernel, (1, 1, 1), 'VALID', dimension_numbers=('NCDHW', 'OIDHW', 'NCDHW'), preferred_element_type=jnp.float32)[0]

def conv_layer(volume, weight):
    padded = jnp.pad(volume, ((0, 0), (1, 1), (1, 1), (1, 1)), mode='wrap')
    return jnp.maximum(conv_taps(padded, weight, volume.shape[0]), 0.0).astype(jnp.bfloat16)

def full_weight(stored):
    width_out = stored.shape[0] // 4
    return stored.reshape(4, width_out, stored.shape[1]).transpose(1, 0, 2).reshape(width_out, 4 * stored.shape[1])

def shrink(volume, weight):
    kernel = weight.reshape(weight.shape[0], volume.shape[0], 2, 2, 2)
    result = lax.conv_general_dilated(volume[None], kernel, (2, 2, 2), 'VALID', dimension_numbers=('NCDHW', 'OIDHW', 'NCDHW'), preferred_element_type=jnp.float32)[0]
    return result.astype(jnp.bfloat16)

def expand(volume, weight, skipped):
    width_in, extent_x, extent_y, extent_z = volume.shape
    width_out = weight.shape[1] // 8
    columns = lax.dot_general(weight, volume.reshape(width_in, -1), (((0,), (0,)), ((), ())), preferred_element_type=jnp.float32)
    spread = columns.reshape(width_out, 2, 2, 2, extent_x, extent_y, extent_z).transpose(0, 4, 1, 5, 2, 6, 3)
    spread = spread.reshape(width_out, 2 * extent_x, 2 * extent_y, 2 * extent_z)
    return (spread + skipped.astype(jnp.float32)).astype(jnp.bfloat16)

def reference(features_in, encode_fine_first, encode_fine_second, reduce_fine, encode_middle_first, encode_middle_second, reduce_middle, bottom_first, bottom_second, expand_middle, decode_middle_first, decode_middle_second, expand_fine, decode_fine_first, decode_fine_second):
    across = math.isqrt(N_YZ)
    volume = to_volume(features_in, across)
    fine_skip = conv_layer(conv_layer(volume, encode_fine_first), encode_fine_second)
    middle = shrink(fine_skip, reduce_fine)
    middle_skip = conv_layer(conv_layer(middle, encode_middle_first), encode_middle_second)
    bottom = shrink(middle_skip, reduce_middle)
    bottom = conv_layer(conv_layer(bottom, full_weight(bottom_first)), full_weight(bottom_second))
    rising = expand(bottom, expand_middle, middle_skip)
    rising = conv_layer(conv_layer(rising, decode_middle_first), decode_middle_second)
    rising = expand(rising, expand_fine, fine_skip)
    rising = conv_layer(conv_layer(rising, decode_fine_first), decode_fine_second)
    return from_volume(rising, across)
```

```python
import math

import jax
import jax.numpy as jnp
import numpy as np
from jax import lax
from jax.experimental import pallas as pl
from jax.experimental.pallas import tpu as pltpu
from jax.sharding import PartitionSpec as P

MESH = pl.DeviceIdType.MESH
BF = jnp.bfloat16
F32 = jnp.float32
YZ8 = [(b, c) for b in (-1, 0, 1) for c in (-1, 0, 1) if (b, c) != (0, 0)]
ALL26 = [
    (a, b, c)
    for a in (-1, 0, 1)
    for b in (-1, 0, 1)
    for c in (-1, 0, 1)
    if (a, b, c) != (0, 0, 0)
]


class Level:
    def __init__(self, width, extent, stride, lanes, group):
        self.width, self.extent, self.stride, self.lanes = width, extent, stride, lanes
        self.planes = extent + 4
        self.share = lanes // 8
        self.per_tile = 128 // self.share
        self.tiles = -(-extent // self.per_tile)
        self.group = group

    def lane(self, y, z):
        return (y + 2) * self.stride + z + 2

    def region(self, step):
        e = self.extent
        return {-1: (0, 1), 0: tuple(range(e)), 1: (e - 2, e - 1)}[step]

    def tables(self):
        pack = np.zeros((self.lanes, self.lanes), np.float32)
        unpack = np.zeros((self.lanes, self.lanes), np.float32)
        for d, (b, c) in enumerate(YZ8):
            cell = 0
            for y in self.region(b):
                for z in self.region(c):
                    slot = d * self.share + cell
                    pack[self.lane(y, z), slot] = 1
                    unpack[slot, self.lane(y - self.extent * b, z - self.extent * c)] = 1
                    cell += 1
        return pack, unpack


FINE = Level(32, 12, 16, 256, 4)
MID = Level(64, 6, 10, 128, 5)
FLAT = 896
OUT1, OUT2 = 640, 384


def constants():
    place = np.zeros((144, 256), np.float32)
    for y in range(12):
        for z in range(12):
            place[y * 12 + z, FINE.lane(y, z)] = 1
    taps = np.zeros((864, 896), np.float32)
    for i in range(32):
        for t in range(27):
            taps[27 * i + t, 32 * t + i] = 1
    eight = np.zeros((256, 256), np.float32)
    for i in range(32):
        for t in range(8):
            eight[8 * i + t, 32 * t + i] = 1
    down = np.zeros((256, 128), np.float32)
    for y in range(6):
        for z in range(6):
            down[FINE.lane(2 * y, 2 * z), MID.lane(y, z)] = 1
    down_bottom = np.zeros((384, 128), np.float32)
    for j in range(3):
        for y in range(3):
            for z in range(3):
                down_bottom[128 * j + MID.lane(2 * y, 2 * z), 9 * j + 3 * y + z] = 1
    up_fine = np.zeros((128, 1024), np.float32)
    for y in range(16):
        for z in range(16):
            part = 2 * (y % 2) + z % 2
            up_fine[(y // 2 + 1) * 10 + z // 2 + 1, 256 * part + 16 * y + z] = 1
    up_mid = np.zeros((128, 512), np.float32)
    for y in range(10):
        for z in range(10):
            part = 2 * (y % 2) + z % 2
            up_mid[9 * (y // 2) + z // 2, 128 * part + 10 * y + z] = 1
    blocks = np.zeros((FLAT, FLAT), np.float32)
    for a in (-1, 0, 1):
        for b in (-1, 0, 1):
            for c in (-1, 0, 1):
                row = 32 * (9 * (a + 1) + 3 * (b + 1) + c + 1)
                for i in range(27):
                    x, y, z = i // 9 - 3 * a + 3, i // 3 % 3 - 3 * b + 3, i % 3 - 3 * c + 3
                    blocks[row + i, 81 * x + 9 * y + z] = 1
    pick = []
    for width in (32, 64):
        table = np.zeros((2 * width, 8 * width), np.float32)
        for a in range(2):
            for o in range(width):
                for part in range(4):
                    table[a * width + o, 8 * o + 4 * a + part] = 1
        pick.append(table)
    fine_pack, fine_unpack = FINE.tables()
    mid_pack, mid_unpack = MID.tables()
    return dict(
        place=place,
        leave=np.pad(place.T, ((0, 0), (0, 112))),
        taps=taps,
        eight=eight,
        down=down,
        down_bottom=down_bottom,
        up_fine=up_fine,
        up_mid=up_mid,
        blocks=blocks,
        pick_fine=pick[0],
        pick_mid=pick[1],
        fine_pack=fine_pack,
        fine_unpack=fine_unpack,
        mid_pack=mid_pack,
        mid_unpack=mid_unpack,
    )


NAMES = (
    "efa", "efb", "rf", "ema", "emb", "rm", "ba", "bb", "xm", "dma", "dmb", "xf", "dfa", "dfb",
)
CONST = tuple(constants().keys())


def ahead(value, shift):
    width = value.shape[1]
    shift = -shift % width
    return value if shift == 0 else pltpu.roll(value, shift, 1)


def dot(a, b):
    return jnp.dot(a, b, preferred_element_type=F32)


def dot_nt(a, b):
    return lax.dot_general(a, b, (((1,), (1,)), ((), ())), preferred_element_type=F32)


def group_of(rows, size):
    return lax.broadcasted_iota(jnp.int32, (rows, 128), 1) // size


def kernel(ngx, nyz, place_of, x_ref, *refs):
    w = dict(zip(NAMES, refs[: len(NAMES)]))
    refs = refs[len(NAMES) :]
    k = dict(zip(CONST, refs[: len(CONST)]))
    refs = refs[len(CONST) :]
    out_ref = refs[0]
    s = dict(zip(SCRATCH, refs[1:]))
    across = math.isqrt(nyz)
    nzh, ny, nx = place_of
    gx, yz = lax.axis_index("gx"), lax.axis_index("yz")

    def device(a, b, c):
        row, col = yz // across, yz % across
        return (
            (gx + a + ngx) % ngx,
            (row + b + across) % across * across + (col + c + across) % across,
        )

    zh, gy, gxx = yz // (ny * nx), yz // nx % ny, yz % nx
    core = gx % 2
    partner = (gx + 1 - 2 * core, yz)
    rs = 1024 // nyz

    def at(z, y, x):
        return z * ny * nx + y * nx + x

    z_peer = ((ngx // 2 - 1 - gx // 2) * 2 + core, at(1 - zh, gy, gxx))
    y_peers = [(gx, at(zh, (gy + d) % ny, gxx)) for d in range(1, ny)]
    x_next = (gx, at(zh, gy, (gxx + 1) % nx))
    x_last = (gx, at(zh, gy, (gxx + nx - 1) % nx))

    barrier = pltpu.get_barrier_semaphore()
    greet = [device(*d) for d in ALL26] + y_peers + [x_next, x_last, partner]
    if nzh == 2:
        greet.append(z_peer)
    for peer in greet:
        pl.semaphore_signal(barrier, inc=1, device_id=peer, device_id_type=MESH)

    started = []

    def send(src, dst, ssem, rsem, peer):
        copy = pltpu.make_async_remote_copy(
            src_ref=src, dst_ref=dst, send_sem=ssem, recv_sem=rsem, device_id=peer, device_id_type=MESH
        )
        copy.start()
        started.append(copy)
        return copy

    for level, ref in ((FINE, s["mid_f"]), (MID, s["mid_m"])):
        n, last = level.lanes, (level.planes - 1) * level.lanes
        ref[:, 0:n] = jnp.zeros((level.width, n), BF)
        ref[:, last : last + n] = jnp.zeros((level.width, n), BF)

    raw_x = s["raw_x"]
    planes = dot(x_ref[...], k["place"][...]).astype(BF)
    for p in range(12):
        raw_x[:, (p + 2) * 256 : (p + 3) * 256] = planes[32 * p : 32 * p + 32]

    def pack(level, raw, message):
        c, e, n = level.width, level.extent, level.lanes
        table = k["fine_pack" if level is FINE else "mid_pack"]
        which = group_of(c, level.share)
        for t in range(level.tiles):
            members = range(t * level.per_tile, min(e, (t + 1) * level.per_tile))
            rows = jnp.concatenate([raw[:, (p + 2) * n : (p + 3) * n] for p in members], axis=0)
            faces = dot(rows, table[...])
            for d in range(8):
                half, base = divmod(d * level.share, 128)
                tile = jnp.zeros((c, 128), F32)
                for q in range(len(members)):
                    part = faces[q * c : (q + 1) * c, 128 * half : 128 * half + 128]
                    tile = jnp.where(which == q, ahead(part, base - q * level.share), tile)
                message[d, t] = tile.astype(BF)

    def exchange(level, raw, message, arrived, ssem, rsem):
        n, e = level.lanes, level.extent
        copies = []
        for m, (a, b, c) in enumerate(ALL26):
            if (b, c) == (0, 0):
                src = raw.at[:, (e * n if a == 1 else 2 * n) : (e * n if a == 1 else 2 * n) + 2 * n]
                dst = raw.at[:, 0 : 2 * n] if a == 1 else raw.at[:, (e + 2) * n : (e + 4) * n]
            else:
                d = YZ8.index((b, c))
                if a == 0:
                    src, dst = message.at[d], arrived.at[1, d]
                else:
                    src = message.at[d, level.tiles - 1 if a == 1 else 0]
                    dst = arrived.at[2 if a == 1 else 0, d, 0]
            copies.append(send(src, dst, ssem.at[m], rsem.at[m], device(a, b, c)))
        return copies

    def unpack(level, raw, arrived, full, copies):
        c, e, n = level.width, level.extent, level.lanes
        table = k["fine_unpack" if level is FINE else "mid_unpack"]
        which = group_of(c, level.share)
        for copy in copies:
            copy.wait_recv()

        def halo(plane):
            p = plane - 2
            slot, tile = 1, p // level.per_tile
            if p < 0:
                slot, tile, p = 2, 0, p + e
            elif p >= e:
                slot, tile, p = 0, 0, p - e
            q = p % level.per_tile
            halves = []
            for half in range(n // 128):
                value = jnp.zeros((c, 128), F32)
                for d in range(8):
                    if d * level.share // 128 == half:
                        base = d * level.share % 128
                        piece = arrived[slot, d, tile].astype(F32)
                        value = jnp.where(
                            which == base // level.share, ahead(piece, q * level.share - base), value
                        )
                halves.append(value)
            return jnp.concatenate(halves, axis=1) if len(halves) > 1 else halves[0]

        step = 4 if level is FINE else 5
        for first in range(0, level.planes, step):
            members = range(first, first + step)
            rows = jnp.concatenate([halo(m) for m in members], axis=0).astype(BF)
            placed = dot(rows, table[...])
            for q, m in enumerate(members):
                own = raw[:, m * n : (m + 1) * n].astype(F32)
                full[:, m * n : (m + 1) * n] = (own + placed[q * c : (q + 1) * c]).astype(BF)

    def conv(level, src, weight, dst):
        c, n = level.width, level.lanes
        width = level.group * n
        cols, sums = (s["cols_f"], s["sums_f"]) if level is FINE else (s["cols_m"], s["sums_m"])

        def one(g, carry):
            lanes = pl.ds(pl.multiple_of(g * width, width), width)
            for ib in range(c // 32):
                rows = src[32 * ib : 32 * ib + 32, lanes].astype(F32)
                for t in range(9):
                    shift = level.stride * (t // 3 - 1) + t % 3 - 1
                    top = 288 * ib + 32 * t
                    cols[top : top + 32, :] = ahead(rows, shift).astype(BF)
            sums[:, lanes] = dot(weight[...], cols[...])
            return carry

        lax.fori_loop(0, level.planes // level.group, one, 0)

        def two(x, carry):
            def lanes(d):
                return pl.ds(pl.multiple_of((x + d) * n, n), n)

            total = sums[0:c, lanes(-1)] + sums[c : 2 * c, lanes(0)] + sums[2 * c : 3 * c, lanes(1)]
            dst[:, lanes(0)] = jnp.maximum(total, 0.0).astype(BF)
            return carry

        lax.fori_loop(1, level.planes - 1, two, 0)

    taps = k["taps"]
    g_ref = s["gathered"]
    own_rows = pl.ds(pl.multiple_of(yz * rs, rs), rs)
    for m, name in enumerate(("ba", "bb")):
        for ib in range(2):
            part = w[name][:, 864 * ib : 864 * ib + 864]
            g_ref[m, ib, own_rows, :] = dot(part, taps[...]).astype(BF)

    pack(FINE, raw_x, s["msg_x"])
    pl.semaphore_wait(barrier, len(greet))
    sent_x = exchange(FINE, raw_x, s["msg_x"], s["got_x"], s["ss"].at[0], s["rs"].at[0])

    def piece(ref, j):
        return ref.at[core, :, pl.ds(pl.multiple_of(j * rs, rs), rs), :]

    nsend = [0]
    waiting = {}

    def pass_on(j, key, peer):
        n = nsend[0]
        nsend[0] += 1
        waiting[key] = send(piece(g_ref, j), piece(g_ref, j), s["gs"].at[n], s["gr"].at[n], peer)

    me = yz
    if nzh == 2:
        pass_on(me, "z", z_peer)
    for d, peer in enumerate(y_peers):
        pass_on(me, ("y", 0, d), peer)

    for n, name in enumerate(("efa", "efb", "dfa", "dfb")):
        flat = dot(w[name][...], taps[...])
        for a in range(3):
            s["wf"][n, 32 * a : 32 * a + 32, :] = ahead(flat, 288 * a)[:, :288].astype(BF)
    lane = lax.broadcasted_iota(jnp.int32, (64, 896), 1)
    for n, name in enumerate(("ema", "emb", "dma", "dmb")):
        low = dot(w[name][:, 0:864], taps[...])
        high = dot(w[name][:, 864:1728], taps[...])
        for a in range(3):
            both = jnp.where(lane < 288, ahead(low, 288 * a), ahead(high, 288 * a - 288))
            s["wm"][n, 64 * a : 64 * a + 64, :] = both[:, :576].astype(BF)
    s["wr"][...] = dot(w["rf"][...], k["eight"][...]).astype(BF)
    for ib in range(2):
        s["wrm"][:, 256 * ib : 256 * ib + 256] = dot(
            w["rm"][:, 256 * ib : 256 * ib + 256], k["eight"][...]
        ).astype(BF)
    for name, table, into, wide in (("xf", "pick_fine", "wx", 256), ("xm", "pick_mid", "wxm", 512)):
        value = w[name][...].astype(F32)
        part = lax.broadcasted_iota(jnp.int32, value.shape, 1) % 4
        rows = jnp.concatenate([jnp.where(part == q, value, 0.0) for q in range(4)], axis=0)
        s[into][...] = dot_nt(k[table][...], rows.astype(BF)).astype(BF)

    if nzh == 2:
        waiting["z"].wait_recv()
        for d, peer in enumerate(y_peers):
            pass_on(at(1 - zh, gy, gxx), ("y", 1, d), peer)

    full_x, mid_f = s["full_x"], s["mid_f"]
    unpack(FINE, raw_x, s["got_x"], full_x, sent_x)
    conv(FINE, full_x, s["wf"].at[0], mid_f)
    raw_e0 = s["raw_e0"]
    conv(FINE, mid_f, s["wf"].at[1], s["e0"])

    def keep_inside(level, src, raw):
        n = level.lanes
        cells = lax.broadcasted_iota(jnp.int32, (1, n), 1)
        y, z = cells // level.stride - 2, cells % level.stride - 2
        inside = (y >= 0) & (y < level.extent) & (z >= 0) & (z < level.extent)
        for p in range(2, level.extent + 2):
            value = src[:, p * n : (p + 1) * n].astype(F32)
            raw[:, p * n : (p + 1) * n] = jnp.where(inside, value, 0.0).astype(BF)

    keep_inside(FINE, s["e0"], raw_e0)

    own = raw_e0[:, 512 : 14 * 256].astype(F32)
    for t in range(4):
        moved = ahead(own, 16 * (t // 2) + t % 2).astype(BF)
        for j in range(6):
            for a in range(2):
                top = 128 * a + 32 * t
                s["cols_r"][top : top + 32, 256 * j : 256 * j + 256] = moved[
                    :, 256 * (2 * j + a) : 256 * (2 * j + a) + 256
                ]
    wide = dot(s["wr"][...], s["cols_r"][...]).astype(BF)
    rows = jnp.concatenate([wide[:, 256 * j : 256 * j + 256] for j in range(6)], axis=0)
    small = dot(rows, k["down"][...]).astype(BF)
    raw_h1 = s["raw_h1"]
    for j in range(6):
        raw_h1[:, (j + 2) * 128 : (j + 3) * 128] = small[64 * j : 64 * j + 64]
    pack(MID, raw_h1, s["msg_h1"])
    sent_h1 = exchange(MID, raw_h1, s["msg_h1"], s["got_m"].at[0], s["ss"].at[1], s["rs"].at[1])
    pack(FINE, raw_e0, s["msg_e0"])
    sent_e0 = exchange(FINE, raw_e0, s["msg_e0"], s["got_e0"], s["ss"].at[2], s["rs"].at[2])

    for z in range(nzh):
        for d in range(ny - 1):
            waiting[("y", z, d)].wait_recv()
    zs = [zh, 1 - zh] if nzh == 2 else [zh]
    for n, z in enumerate(zs):
        for d in range(ny):
            j = at(z, (gy + d) % ny, gxx)
            pass_on(j, ("x+", n, d), x_next)
            if nx > 2:
                pass_on(j, ("x-", n, d), x_last)

    full_m, mid_m = s["full_m"], s["mid_m"]
    unpack(MID, raw_h1, s["got_m"].at[0], full_m, sent_h1)
    conv(MID, full_m, s["wm"].at[0], mid_m)
    conv(MID, mid_m, s["wm"].at[1], s["e1"])
    raw_e1 = s["raw_e1"]
    keep_inside(MID, s["e1"], raw_e1)

    own = raw_e1[:, 256 : 8 * 128].astype(F32)
    for t in range(4):
        moved = ahead(own, 10 * (t // 2) + t % 2).astype(BF)
        for j in range(3):
            for a in range(2):
                for ib in range(2):
                    top = 256 * ib + 128 * a + 32 * t
                    s["cols_rm"][top : top + 32, 128 * j : 128 * j + 128] = moved[
                        32 * ib : 32 * ib + 32, 128 * (2 * j + a) : 128 * (2 * j + a) + 128
                    ]
    wide = dot(s["wrm"][...], s["cols_rm"][...]).astype(BF)
    cells = dot(wide, k["down_bottom"][...])
    which = group_of(64, 32)
    tile = jnp.zeros((64, 128), F32)
    for q in range(4):
        tile = jnp.where(which == q, ahead(cells[64 * q : 64 * q + 64], -32 * q), tile)
    s["msg_b"][...] = tile.astype(BF)
    got_b = s["got_b"]
    got_b[13] = tile.astype(BF)
    sent_b = []
    for m, (a, b, c) in enumerate(ALL26):
        slot = 9 * (a + 1) + 3 * (b + 1) + c + 1
        sent_b.append(
            send(s["msg_b"], got_b.at[slot], s["ss"].at[3, m], s["rs"].at[3, m], device(a, b, c))
        )
    pack(MID, raw_e1, s["msg_e1"])
    sent_e1 = exchange(MID, raw_e1, s["msg_e1"], s["got_m"].at[1], s["ss"].at[4], s["rs"].at[4])

    for n in range(len(zs)):
        for d in range(ny):
            waiting[("x+", n, d)].wait_recv()
            if nx > 2:
                waiting[("x-", n, d)].wait_recv()
    far = []
    if nx > 2:
        for n, z in enumerate(zs):
            for d in range(ny):
                y = (gy + d) % ny
                if n == 0:
                    pass_on(at(z, y, (gxx + nx - 1) % nx), ("f", n, d), x_next)
                else:
                    pass_on(at(z, y, (gxx + 1) % nx), ("f", n, d), x_last)
                far.append(("f", n, d))
    for key in far:
        waiting[key].wait_recv()
    half = pltpu.make_async_remote_copy(
        src_ref=g_ref.at[core],
        dst_ref=g_ref.at[core],
        send_sem=s["ps"].at[0],
        recv_sem=s["ps"].at[1],
        device_id=partner,
        device_id_type=MESH,
    )
    half.start()

    for copy in sent_b:
        copy.wait_recv()
    for q in range(4):
        tiles = []
        for t in range(7):
            tile = jnp.zeros((64, 128), F32)
            for b in range(4):
                if 4 * t + b < 27:
                    tile = jnp.where(
                        which == b, ahead(got_b[4 * t + b].astype(F32), 32 * (q - b)), tile
                    )
            tiles.append(tile.astype(BF))
        s["b0"][64 * q : 64 * q + 64, :] = dot(jnp.concatenate(tiles, axis=1), k["blocks"][...]).astype(BF)
    half.wait()
    cols_b, acc = s["cols_b"], s["acc"]
    cols_b[864:896, :] = jnp.zeros((32, OUT1), BF)

    def bottom(src, m, dst, width):
        acc[:, :width] = jnp.zeros((256, width), F32)

        def one(kk, carry):
            rows = src[pl.ds(pl.multiple_of(kk * 32, 32), 32), :].astype(F32)
            for t in range(27):
                shift = 81 * (t // 9) + 9 * (t // 3 % 3) + t % 3
                cols_b[32 * t : 32 * t + 32, :width] = ahead(rows, shift)[:, :width].astype(BF)
            lhs = g_ref[m, kk % 2, pl.ds(pl.multiple_of(kk // 2 * 256, 256), 256), :]
            acc[:, :width] += dot(lhs, cols_b[:, :width])
            return carry

        lax.fori_loop(0, 8, one, 0)
        dst[...] = jnp.maximum(acc[:, :width], 0.0).astype(BF)

    bottom(s["b0"], 0, s["b1"], OUT1)
    bottom(s["b1"], 1, s["b2"], OUT2)

    full_e1 = s["full_e1"]
    unpack(MID, raw_e1, s["got_m"].at[1], full_e1, sent_e1)
    base = s["b2"][...].astype(F32)
    for j in range(5):
        spread = dot(ahead(base, 81 * j)[:, :128].astype(BF), k["up_mid"][...]).astype(BF)
        rows = jnp.concatenate([spread[:, 128 * q : 128 * q + 128] for q in range(4)], axis=0)
        risen = dot(s["wxm"][...], rows)
        for a in range(2):
            lanes = slice((2 * j + a) * 128, (2 * j + a + 1) * 128)
            total = risen[64 * a : 64 * a + 64] + full_e1[:, lanes].astype(F32)
            full_m[:, lanes] = total.astype(BF)
    conv(MID, full_m, s["wm"].at[2], mid_m)
    conv(MID, mid_m, s["wm"].at[3], s["f1"])
    raw_f1 = s["raw_f1"]
    keep_inside(MID, s["f1"], raw_f1)
    pack(MID, raw_f1, s["msg_f1"])
    sent_f1 = exchange(MID, raw_f1, s["msg_f1"], s["got_m"].at[2], s["ss"].at[5], s["rs"].at[5])

    full_e0 = s["full_e0"]
    unpack(FINE, raw_e0, s["got_e0"], full_e0, sent_e0)
    unpack(MID, raw_f1, s["got_m"].at[2], s["full_f1"], sent_f1)
    for j in range(8):
        spread = dot(s["full_f1"][:, (j + 1) * 128 : (j + 2) * 128], k["up_fine"][...]).astype(BF)
        rows = jnp.concatenate([spread[:, 256 * q : 256 * q + 256] for q in range(4)], axis=0)
        risen = dot(s["wx"][...], rows)
        for a in range(2):
            lanes = slice((2 * j + a) * 256, (2 * j + a + 1) * 256)
            total = risen[32 * a : 32 * a + 32] + full_e0[:, lanes].astype(F32)
            full_x[:, lanes] = total.astype(BF)
    conv(FINE, full_x, s["wf"].at[2], mid_f)
    conv(FINE, mid_f, s["wf"].at[3], s["e0"])
    rows = jnp.concatenate([s["e0"][:, (p + 2) * 256 : (p + 3) * 256] for p in range(12)], axis=0)
    out_ref[...] = dot(rows, k["leave"][...])[:, :144].astype(BF)
    for copy in started:
        copy.wait_send()


def scratch(nyz, place_of):
    nzh, ny, nx = place_of
    fine, mid = (32, 16 * 256), (64, 10 * 128)
    count = 1 + nzh * (ny - 1) + 3 * nzh * ny
    vm = lambda *shape: pltpu.VMEM(shape, BF)
    return dict(
        raw_x=vm(*fine), full_x=vm(*fine), mid_f=vm(*fine), e0=vm(*fine), raw_e0=vm(*fine), full_e0=vm(*fine),
        raw_h1=vm(*mid), full_m=vm(*mid), mid_m=vm(*mid), e1=vm(*mid), raw_e1=vm(*mid), full_e1=vm(*mid),
        f1=vm(*mid), raw_f1=vm(*mid), full_f1=vm(*mid),
        msg_x=vm(8, 3, 32, 128), msg_e0=vm(8, 3, 32, 128), got_x=vm(3, 8, 3, 32, 128), got_e0=vm(3, 8, 3, 32, 128),
        msg_h1=vm(8, 1, 64, 128), msg_e1=vm(8, 1, 64, 128), msg_f1=vm(8, 1, 64, 128), got_m=vm(3, 3, 8, 1, 64, 128),
        msg_b=vm(64, 128), got_b=vm(27, 64, 128),
        b0=vm(256, FLAT), b1=vm(256, OUT1), b2=vm(256, OUT2),
        wf=vm(4, 96, 288), wm=vm(4, 192, 576), wr=vm(64, 256), wrm=vm(256, 512), wx=vm(64, 256), wxm=vm(128, 1024),
        gathered=vm(2, 2, 1024, 896),
        cols_f=vm(288, 1024), cols_m=vm(576, 640), cols_r=vm(256, 1536), cols_rm=vm(512, 384), cols_b=vm(896, OUT1),
        sums_f=pltpu.VMEM((96, 16 * 256), F32), sums_m=pltpu.VMEM((192, 1280), F32), acc=pltpu.VMEM((256, OUT1), F32),
        ss=pltpu.SemaphoreType.DMA((6, 26)), rs=pltpu.SemaphoreType.DMA((6, 26)),
        gs=pltpu.SemaphoreType.DMA((count,)), gr=pltpu.SemaphoreType.DMA((count,)), ps=pltpu.SemaphoreType.DMA((2,)),
    )


SCRATCH = tuple(scratch(64, (2, 8, 4)))


def solution(mesh):
    ngx, nyz = mesh.shape["gx"], mesh.shape["yz"]
    place_of = (2, 8, 4) if nyz == 64 else (1, math.isqrt(nyz), math.isqrt(nyz))
    tables = {name: np.asarray(value, BF) for name, value in constants().items()}

    def body(features_in, *weights):
        planes = features_in[0].transpose(1, 0, 2).reshape(384, 144)
        result = pl.pallas_call(
            lambda *refs: kernel(ngx, nyz, place_of, *refs),
            name="unet",
            out_shape=jax.ShapeDtypeStruct((384, 144), BF),
            in_specs=[pl.BlockSpec(memory_space=pltpu.VMEM)] * (1 + len(NAMES) + len(CONST)),
            out_specs=pl.BlockSpec(memory_space=pltpu.VMEM),
            scratch_shapes=list(scratch(nyz, place_of).values()),
            compiler_params=pltpu.CompilerParams(
                collective_id=0, has_side_effects=True, vmem_limit_bytes=60 * 2**20
            ),
        )(planes, *weights, *(jnp.asarray(tables[name]) for name in CONST))
        return result.reshape(12, 32, 144).transpose(1, 0, 2)[None]

    placed = tuple(
        P("yz", None, "gx", None) if i == 0 else P("yz", None) if i in (7, 8) else P() for i in range(15)
    )
    return jax.shard_map(
        body, mesh=mesh, in_specs=placed, out_specs=P("yz", None, "gx", None), check_vma=False
    )
```

```python
import math

import jax
import jax.numpy as jnp
import numpy as np
from jax import lax
from jax.experimental import pallas as pl
from jax.experimental.pallas import tpu as pltpu
from jax.sharding import PartitionSpec as P

MESH = pl.DeviceIdType.MESH
BF = jnp.bfloat16
F32 = jnp.float32
YZ8 = [(b, c) for b in (-1, 0, 1) for c in (-1, 0, 1) if (b, c) != (0, 0)]
ALL26 = [
    (a, b, c)
    for a in (-1, 0, 1)
    for b in (-1, 0, 1)
    for c in (-1, 0, 1)
    if (a, b, c) != (0, 0, 0)
]


CORNERS = [d for d, (b, c) in enumerate(YZ8) if b and c]


class Level:
    def __init__(self, width, extent, stride, lanes, group):
        self.width, self.extent, self.stride, self.lanes = width, extent, stride, lanes
        self.planes = extent + 4
        self.share = lanes // 8
        self.per_tile = 128 // self.share
        self.tiles = -(-extent // self.per_tile)
        self.group = group
        self.fold = width // 16
        self.span = 128 // self.fold

    def lane(self, y, z):
        return (y + 2) * self.stride + z + 2

    def region(self, step):
        e = self.extent
        return {-1: (0, 1), 0: tuple(range(e)), 1: (e - 2, e - 1)}[step]

    def tables(self):
        pack = np.zeros((self.lanes, self.lanes), np.float32)
        unpack = np.zeros((self.lanes, self.lanes), np.float32)
        for d, (b, c) in enumerate(YZ8):
            cell = 0
            for y in self.region(b):
                for z in self.region(c):
                    slot = d * self.share + cell
                    pack[self.lane(y, z), slot] = 1
                    unpack[slot, self.lane(y - self.extent * b, z - self.extent * c)] = 1
                    cell += 1
        return pack, unpack


FINE = Level(32, 12, 16, 256, 4)
MID = Level(64, 6, 10, 128, 5)
FLAT = 896
OUT1, OUT2 = 640, 384


def constants():
    place = np.zeros((144, 256), np.float32)
    for y in range(12):
        for z in range(12):
            place[y * 12 + z, FINE.lane(y, z)] = 1
    eight = np.zeros((256, 256), np.float32)
    for i in range(32):
        for t in range(8):
            eight[8 * i + t, 32 * t + i] = 1
    down = np.zeros((256, 128), np.float32)
    for y in range(6):
        for z in range(6):
            down[FINE.lane(2 * y, 2 * z), MID.lane(y, z)] = 1
    down_bottom = np.zeros((384, 128), np.float32)
    for j in range(3):
        for y in range(3):
            for z in range(3):
                down_bottom[128 * j + MID.lane(2 * y, 2 * z), 9 * j + 3 * y + z] = 1
    up_fine = np.zeros((128, 1024), np.float32)
    for y in range(16):
        for z in range(16):
            part = 2 * (y % 2) + z % 2
            up_fine[(y // 2 + 1) * 10 + z // 2 + 1, 256 * part + 16 * y + z] = 1
    up_mid = np.zeros((128, 512), np.float32)
    for y in range(10):
        for z in range(10):
            part = 2 * (y % 2) + z % 2
            up_mid[9 * (y // 2) + z // 2, 128 * part + 10 * y + z] = 1
    pick = []
    for width in (32, 64):
        table = np.zeros((2 * width, 8 * width), np.float32)
        for a in range(2):
            for o in range(width):
                for part in range(4):
                    table[a * width + o, 8 * o + 4 * a + part] = 1
        pick.append(table)
    fine_pack, fine_unpack = FINE.tables()
    mid_pack, mid_unpack = MID.tables()
    return dict(
        place=place,
        leave=np.pad(place.T, ((0, 0), (0, 112))),
        eight=eight,
        down=down,
        down_bottom=down_bottom,
        up_fine=up_fine,
        up_mid=up_mid,
        pick_fine=pick[0],
        pick_mid=pick[1],
        fine_pack=fine_pack,
        fine_unpack=fine_unpack,
        mid_pack=mid_pack,
        mid_unpack=mid_unpack,
    )


NAMES = (
    "efa", "efb", "rf", "ema", "emb", "rm", "ba", "bb", "xm", "dma", "dmb", "xf", "dfa", "dfb",
)
CONST = tuple(constants().keys())


def ahead(value, shift):
    width = value.shape[1]
    shift = -shift % width
    return value if shift == 0 else pltpu.roll(value, shift, 1)


def dot(a, b):
    return jnp.dot(a, b, preferred_element_type=F32)


def dot_nt(a, b):
    return lax.dot_general(a, b, (((1,), (1,)), ((), ())), preferred_element_type=F32)


def group_of(rows, size):
    return lax.broadcasted_iota(jnp.int32, (rows, 128), 1) // size


def kernel(ngx, nyz, place_of, x_ref, *refs):
    w = dict(zip(NAMES, refs[: len(NAMES)]))
    refs = refs[len(NAMES) :]
    k = dict(zip(CONST, refs[: len(CONST)]))
    refs = refs[len(CONST) :]
    out_ref = refs[0]
    s = dict(zip(SCRATCH, refs[1:]))
    across = math.isqrt(nyz)
    nzh, ny, nx = place_of
    gx, yz = lax.axis_index("gx"), lax.axis_index("yz")

    def device(a, b, c):
        row, col = yz // across, yz % across
        return (
            (gx + a + ngx) % ngx,
            (row + b + across) % across * across + (col + c + across) % across,
        )

    zh, gy, gxx = yz // (ny * nx), yz // nx % ny, yz % nx
    core = gx % 2
    partner = (gx + 1 - 2 * core, yz)
    rs = 1024 // nyz

    def at(z, y, x):
        return z * ny * nx + y * nx + x

    z_peer = ((ngx // 2 - 1 - gx // 2) * 2 + core, at(1 - zh, gy, gxx))
    y_peers = [(gx, at(zh, (gy + d) % ny, gxx)) for d in range(1, ny)]
    x_next = (gx, at(zh, gy, (gxx + 1) % nx))
    x_last = (gx, at(zh, gy, (gxx + nx - 1) % nx))

    barrier = pltpu.get_barrier_semaphore()
    greet = [device(*d) for d in ALL26] + y_peers + [x_next, x_last, partner]
    if nzh == 2:
        greet.append(z_peer)
    for peer in greet:
        pl.semaphore_signal(barrier, inc=1, device_id=peer, device_id_type=MESH)

    def box_of(name):
        return {part: s[name + "_" + part] for part in ("face", "wing", "corner", "end") if name + "_" + part in s}

    started = []

    def send(src, dst, ssem, rsem, peer):
        copy = pltpu.make_async_remote_copy(
            src_ref=src, dst_ref=dst, send_sem=ssem, recv_sem=rsem, device_id=peer, device_id_type=MESH
        )
        copy.start()
        started.append(copy)
        return copy

    for level, ref in ((FINE, s["mid_f"]), (MID, s["mid_m"])):
        n, last = level.lanes, (level.planes - 1) * level.lanes
        ref[:, 0:n] = jnp.zeros((level.width, n), BF)
        ref[:, last : last + n] = jnp.zeros((level.width, n), BF)

    raw_x = s["raw_x"]
    planes = dot(x_ref[...], k["place"][...]).astype(BF)
    for p in range(12):
        raw_x[:, (p + 2) * 256 : (p + 3) * 256] = planes[32 * p : 32 * p + 32]

    def folded(level, value, start):
        which = group_of(16, level.span)
        tile = jnp.zeros((16, 128), F32)
        for h in range(level.fold):
            tile = jnp.where(which == h, ahead(value[16 * h : 16 * h + 16], start - level.span * h), tile)
        return tile.astype(BF)

    def unfolded(level, value, start):
        value = value.astype(F32)
        return jnp.concatenate([ahead(value, level.span * h - start) for h in range(level.fold)], axis=0)

    def pack(level, raw, box):
        c, e, n = level.width, level.extent, level.lanes
        table = k["fine_pack" if level is FINE else "mid_pack"]
        which = group_of(c, level.share)
        which4 = group_of(c, 4)
        corners = [jnp.zeros((c, 128), F32)] * 8
        for t in range(level.tiles):
            members = range(t * level.per_tile, min(e, (t + 1) * level.per_tile))
            rows = jnp.concatenate([raw[:, (p + 2) * n : (p + 3) * n] for p in members], axis=0)
            faces = dot(rows, table[...])
            for d in range(8):
                half, base = divmod(d * level.share, 128)
                tile = jnp.zeros((c, 128), F32)
                for q, p in enumerate(members):
                    part = faces[q * c : (q + 1) * c, 128 * half : 128 * half + 128]
                    tile = jnp.where(which == q, ahead(part, base - q * level.share), tile)
                    if d in CORNERS:
                        corners[d] = jnp.where(which4 == p, ahead(part, base - 4 * p), corners[d])
                if d not in CORNERS:
                    box["face"][d, t] = tile.astype(BF)
                if t == level.tiles - 1:
                    box["wing"][1, d] = folded(level, tile, 64)
                if t == 0:
                    box["wing"][0, d] = folded(level, tile, 0)
        for d in CORNERS:
            box["corner"][d] = folded(level, corners[d], 0)
        if level is MID:
            low = lax.broadcasted_iota(jnp.int32, (c, 128), 1) < 64
            for side, first in ((1, e), (0, 2)):
                a = raw[:, first * n : (first + 1) * n].astype(F32)
                b = raw[:, (first + 1) * n : (first + 2) * n].astype(F32)
                box["end"][side] = jnp.where(low, ahead(a, 22), ahead(b, 22 - 64)).astype(BF)

    def exchange(level, raw, box, got, ssem, rsem):
        n, e = level.lanes, level.extent
        copies = []
        for m, (a, b, c) in enumerate(ALL26):
            side = 1 if a == 1 else 0
            if (b, c) == (0, 0):
                if level is MID:
                    src, dst = box["end"].at[side], got["end"].at[side]
                elif a == 1:
                    src, dst = raw.at[:, e * n : (e + 2) * n], raw.at[:, 0 : 2 * n]
                else:
                    src, dst = raw.at[:, 2 * n : 4 * n], raw.at[:, (e + 2) * n : (e + 4) * n]
            else:
                d = YZ8.index((b, c))
                if a != 0:
                    src, dst = box["wing"].at[side, d], got["wing"].at[side, d]
                elif d in CORNERS:
                    src, dst = box["corner"].at[d], got["corner"].at[d]
                else:
                    src, dst = box["face"].at[d], got["face"].at[d]
            copies.append(send(src, dst, ssem.at[m], rsem.at[m], device(a, b, c)))
        return copies

    def unpack(level, raw, got, full, copies):
        c, e, n = level.width, level.extent, level.lanes
        table = k["fine_unpack" if level is FINE else "mid_unpack"]
        which = group_of(c, level.share)
        for copy in copies:
            copy.wait_recv()
        if level is MID:
            lane = lax.broadcasted_iota(jnp.int32, (c, 128), 1)
            mine = (lane >= 22) & (lane < 86)
            for side, first in ((1, 0), (0, e + 2)):
                value = got["end"][side].astype(F32)
                for q in range(2):
                    lanes = slice((first + q) * n, (first + q + 1) * n)
                    raw[:, lanes] = jnp.where(mine, ahead(value, 64 * q - 22), 0.0).astype(BF)
        corner = {d: unfolded(level, got["corner"][d], 0) for d in CORNERS}
        wing = {
            (side, d): unfolded(level, got["wing"][side, d], 64 * side) for side in range(2) for d in range(8)
        }

        def halo(plane):
            p = plane - 2
            halves = []
            for half in range(n // 128):
                value = jnp.zeros((c, 128), F32)
                for d in range(8):
                    if d * level.share // 128 != half:
                        continue
                    base = d * level.share % 128
                    if p < 0:
                        piece, start = wing[1, d], (p + e) % level.per_tile * level.share
                    elif p >= e:
                        piece, start = wing[0, d], (p - e) * level.share
                    elif d in CORNERS:
                        piece, start = corner[d], 4 * p
                    else:
                        piece = got["face"][d, p // level.per_tile].astype(F32)
                        start = p % level.per_tile * level.share
                    value = jnp.where(which == base // level.share, ahead(piece, start - base), value)
                halves.append(value)
            return jnp.concatenate(halves, axis=1) if len(halves) > 1 else halves[0]

        step = 4 if level is FINE else 5
        for first in range(0, level.planes, step):
            members = range(first, first + step)
            rows = jnp.concatenate([halo(m) for m in members], axis=0).astype(BF)
            placed = dot(rows, table[...])
            for q, m in enumerate(members):
                own = raw[:, m * n : (m + 1) * n].astype(F32)
                full[:, m * n : (m + 1) * n] = (own + placed[q * c : (q + 1) * c]).astype(BF)

    def conv(level, src, weight, dst):
        c, n = level.width, level.lanes
        width = level.group * n
        cols, sums = (s["cols_f"], s["sums_f"]) if level is FINE else (s["cols_m"], s["sums_m"])

        def one(g, carry):
            lanes = pl.ds(pl.multiple_of(g * width, width), width)
            for ib in range(c // 32):
                rows = src[32 * ib : 32 * ib + 32, lanes].astype(F32)
                for t in range(9):
                    shift = level.stride * (t // 3 - 1) + t % 3 - 1
                    top = 288 * ib + 32 * t
                    cols[top : top + 32, :] = ahead(rows, shift).astype(BF)
            sums[:, lanes] = dot(weight[...], cols[...])
            return carry

        lax.fori_loop(0, level.planes // level.group, one, 0)

        def two(x, carry):
            def lanes(d):
                return pl.ds(pl.multiple_of((x + d) * n, n), n)

            total = sums[0:c, lanes(-1)] + sums[c : 2 * c, lanes(0)] + sums[2 * c : 3 * c, lanes(1)]
            dst[:, lanes(0)] = jnp.maximum(total, 0.0).astype(BF)
            return carry

        lax.fori_loop(1, level.planes - 1, two, 0)

    taps = s["taps"]
    column = lax.broadcasted_iota(jnp.int32, (1, 896), 1)
    wanted = jnp.where(column < 864, 27 * (column & 31) + (column >> 5), -1)
    row = lax.broadcasted_iota(jnp.int32, (32, 896), 0)

    def tap_rows(n, carry):
        taps[pl.ds(pl.multiple_of(n * 32, 32), 32), :] = jnp.where(row + 32 * n == wanted, 1.0, 0.0).astype(BF)
        return carry

    lax.fori_loop(0, 27, tap_rows, 0)
    g_ref = s["gathered"]
    own_rows = pl.ds(pl.multiple_of(yz * rs, rs), rs)
    for m, name in enumerate(("ba", "bb")):
        for ib in range(2):
            part = w[name][:, 864 * ib : 864 * ib + 864]
            g_ref[m, ib, own_rows, :] = dot(part, taps[...]).astype(BF)

    pack(FINE, raw_x, box_of("msg_x"))
    pl.semaphore_wait(barrier, len(greet))
    sent_x = exchange(FINE, raw_x, box_of("msg_x"), box_of("got_x"), s["ss"].at[0], s["rs"].at[0])

    def piece(ref, j):
        return ref.at[core, :, pl.ds(pl.multiple_of(j * rs, rs), rs), :]

    nsend = [0]
    waiting = {}

    def pass_on(j, key, peer):
        n = nsend[0]
        nsend[0] += 1
        waiting[key] = send(piece(g_ref, j), piece(g_ref, j), s["gs"].at[n], s["gr"].at[n], peer)

    zs = [zh, 1 - zh] if nzh == 2 else [zh]

    def along_y(i):
        for d, peer in enumerate(y_peers):
            pass_on(at(zs[i], gy, gxx), ("y", i, d + 1), peer)

    def along_x(i, d, local):
        j = at(zs[i], (gy - d + ny) % ny, gxx)
        pass_on(j, ("x+", i, d), x_next)
        if nx > 2:
            pass_on(j, ("x-", i, d), x_last)
        if not local:
            pass_on(j, ("p", i, d, 0), partner)

    if nzh == 2:
        pass_on(yz, "z", z_peer)
    along_y(0)
    along_x(0, 0, True)

    for n, name in enumerate(("efa", "efb", "dfa", "dfb")):
        flat = dot(w[name][...], taps[...])
        for a in range(3):
            s["wf"][n, 32 * a : 32 * a + 32, :] = ahead(flat, 288 * a)[:, :288].astype(BF)
    lane = lax.broadcasted_iota(jnp.int32, (64, 896), 1)
    for n, name in enumerate(("ema", "emb", "dma", "dmb")):
        low = dot(w[name][:, 0:864], taps[...])
        high = dot(w[name][:, 864:1728], taps[...])
        for a in range(3):
            both = jnp.where(lane < 288, ahead(low, 288 * a), ahead(high, 288 * a - 288))
            s["wm"][n, 64 * a : 64 * a + 64, :] = both[:, :576].astype(BF)
    s["wr"][...] = dot(w["rf"][...], k["eight"][...]).astype(BF)
    for ib in range(2):
        s["wrm"][:, 256 * ib : 256 * ib + 256] = dot(
            w["rm"][:, 256 * ib : 256 * ib + 256], k["eight"][...]
        ).astype(BF)
    for name, table, into, wide in (("xf", "pick_fine", "wx", 256), ("xm", "pick_mid", "wxm", 512)):
        value = w[name][...].astype(F32)
        part = lax.broadcasted_iota(jnp.int32, value.shape, 1) % 4
        rows = jnp.concatenate([jnp.where(part == q, value, 0.0) for q in range(4)], axis=0)
        s[into][...] = dot_nt(k[table][...], rows.astype(BF)).astype(BF)

    column = lax.broadcasted_iota(jnp.int32, (32, FLAT), 1)
    cell = lax.broadcasted_iota(jnp.int32, (32, 1), 0)
    cx = (cell * 57) >> 9
    cy = ((cell - 9 * cx) * 11) >> 5
    offset = jnp.where(cell < 27, 72 * cx + 6 * cy + cell, -4096)
    blocks = s["blocks"]
    blocks[864:896, :] = jnp.zeros((32, FLAT), BF)

    def block_rows(b, carry):
        first = 81 * 3 * (2 - b // 9) + 9 * 3 * (2 - b // 3 % 3) + 3 * (2 - b % 3)
        blocks[pl.ds(pl.multiple_of(b * 32, 32), 32), :] = jnp.where(column == offset + first, 1.0, 0.0).astype(BF)
        return carry

    lax.fori_loop(0, 27, block_rows, 0)

    def step_y(i):
        for d in sorted(range(1, ny), key=lambda d: min(d, ny - d)):
            waiting["y", i, d].wait_recv()
            along_x(i, d, False)

    if nzh == 2:
        waiting["z"].wait_recv()
        along_y(1)
        along_x(1, 0, False)

    full_x, mid_f = s["full_x"], s["mid_f"]
    step_y(0)
    unpack(FINE, raw_x, box_of("got_x"), full_x, sent_x)
    conv(FINE, full_x, s["wf"].at[0], mid_f)
    raw_e0 = s["raw_e0"]
    conv(FINE, mid_f, s["wf"].at[1], s["e0"])

    def keep_inside(level, src, raw):
        n = level.lanes
        cells = lax.broadcasted_iota(jnp.int32, (1, n), 1)
        y, z = cells // level.stride - 2, cells % level.stride - 2
        inside = (y >= 0) & (y < level.extent) & (z >= 0) & (z < level.extent)
        for p in range(2, level.extent + 2):
            value = src[:, p * n : (p + 1) * n].astype(F32)
            raw[:, p * n : (p + 1) * n] = jnp.where(inside, value, 0.0).astype(BF)

    keep_inside(FINE, s["e0"], raw_e0)

    own = raw_e0[:, 512 : 14 * 256].astype(F32)
    for t in range(4):
        moved = ahead(own, 16 * (t // 2) + t % 2).astype(BF)
        for j in range(6):
            for a in range(2):
                top = 128 * a + 32 * t
                s["cols_r"][top : top + 32, 256 * j : 256 * j + 256] = moved[
                    :, 256 * (2 * j + a) : 256 * (2 * j + a) + 256
                ]
    wide = dot(s["wr"][...], s["cols_r"][...]).astype(BF)
    rows = jnp.concatenate([wide[:, 256 * j : 256 * j + 256] for j in range(6)], axis=0)
    small = dot(rows, k["down"][...]).astype(BF)
    raw_h1 = s["raw_h1"]
    for j in range(6):
        raw_h1[:, (j + 2) * 128 : (j + 3) * 128] = small[64 * j : 64 * j + 64]
    pack(MID, raw_h1, box_of("msg_h1"))
    sent_h1 = exchange(MID, raw_h1, box_of("msg_h1"), box_of("got_h1"), s["ss"].at[1], s["rs"].at[1])
    if nzh == 2:
        step_y(1)

    full_m, mid_m = s["full_m"], s["mid_m"]
    unpack(MID, raw_h1, box_of("got_h1"), full_m, sent_h1)
    conv(MID, full_m, s["wm"].at[0], mid_m)
    conv(MID, mid_m, s["wm"].at[1], s["e1"])
    raw_e1 = s["raw_e1"]
    keep_inside(MID, s["e1"], raw_e1)

    own = raw_e1[:, 256 : 8 * 128].astype(F32)
    for t in range(4):
        moved = ahead(own, 10 * (t // 2) + t % 2).astype(BF)
        for j in range(3):
            for a in range(2):
                for ib in range(2):
                    top = 256 * ib + 128 * a + 32 * t
                    s["cols_rm"][top : top + 32, 128 * j : 128 * j + 128] = moved[
                        32 * ib : 32 * ib + 32, 128 * (2 * j + a) : 128 * (2 * j + a) + 128
                    ]
    wide = dot(s["wrm"][...], s["cols_rm"][...]).astype(BF)
    cells = dot(wide, k["down_bottom"][...])
    which = group_of(64, 32)
    tile = jnp.zeros((64, 128), F32)
    for q in range(4):
        tile = jnp.where(which == q, ahead(cells[64 * q : 64 * q + 64], -32 * q), tile)
    s["msg_b"][...] = tile.astype(BF)
    got_b = s["got_b"]
    got_b[13] = tile.astype(BF)
    sent_b = []
    for m, (a, b, c) in enumerate(ALL26):
        slot = 9 * (a + 1) + 3 * (b + 1) + c + 1
        sent_b.append(
            send(s["msg_b"], got_b.at[slot], s["ss"].at[3, m], s["rs"].at[3, m], device(a, b, c))
        )
    pack(MID, raw_e1, box_of("msg_e1"))
    sent_e1 = exchange(MID, raw_e1, box_of("msg_e1"), box_of("got_e1"), s["ss"].at[4], s["rs"].at[4])

    order = [(i, d) for i in range(nzh) for d in sorted(range(ny), key=lambda d: min(d, ny - d))]
    for i, d in order:
        y = (gy - d + ny) % ny
        waiting["x+", i, d].wait_recv()
        j = at(zs[i], y, (gxx + nx - 1) % nx)
        if nx > 2 and i == 0:
            pass_on(j, ("f", i, d), x_next)
        pass_on(j, ("p", i, d, 1), partner)
        if nx > 2:
            waiting["x-", i, d].wait_recv()
            j = at(zs[i], y, (gxx + 1) % nx)
            if i == 1:
                pass_on(j, ("f", i, d), x_last)
            pass_on(j, ("p", i, d, 2), partner)
    pack(FINE, raw_e0, box_of("msg_e0"))
    sent_e0 = exchange(FINE, raw_e0, box_of("msg_e0"), box_of("got_e0"), s["ss"].at[2], s["rs"].at[2])
    if nx > 2:
        for i, d in order:
            waiting["f", i, d].wait_recv()
            pass_on(at(zs[i], (gy - d + ny) % ny, (gxx + 2) % nx), ("p", i, d, 3), partner)

    for copy in sent_b:
        copy.wait_recv()
    for q in range(4):
        tiles = []
        for t in range(7):
            tile = jnp.zeros((64, 128), F32)
            for b in range(4):
                if 4 * t + b < 27:
                    tile = jnp.where(
                        which == b, ahead(got_b[4 * t + b].astype(F32), 32 * (q - b)), tile
                    )
            tiles.append(tile.astype(BF))
        s["b0"][64 * q : 64 * q + 64, :] = dot(jnp.concatenate(tiles, axis=1), blocks[...]).astype(BF)
    for key, copy in waiting.items():
        if key[0] == "p":
            copy.wait_recv()
    cols_b, acc = s["cols_b"], s["acc"]
    cols_b[864:896, :] = jnp.zeros((32, OUT1), BF)

    def bottom(src, m, dst, width):
        acc[:, :width] = jnp.zeros((256, width), F32)

        def one(kk, carry):
            rows = src[pl.ds(pl.multiple_of(kk * 32, 32), 32), :].astype(F32)
            for t in range(27):
                shift = 81 * (t // 9) + 9 * (t // 3 % 3) + t % 3
                cols_b[32 * t : 32 * t + 32, :width] = ahead(rows, shift)[:, :width].astype(BF)
            lhs = g_ref[m, kk % 2, pl.ds(pl.multiple_of(kk // 2 * 256, 256), 256), :]
            acc[:, :width] += dot(lhs, cols_b[:, :width])
            return carry

        lax.fori_loop(0, 8, one, 0)
        dst[...] = jnp.maximum(acc[:, :width], 0.0).astype(BF)

    bottom(s["b0"], 0, s["b1"], OUT1)
    bottom(s["b1"], 1, s["b2"], OUT2)

    full_e1 = s["full_e1"]
    unpack(MID, raw_e1, box_of("got_e1"), full_e1, sent_e1)
    base = s["b2"][...].astype(F32)
    for j in range(5):
        spread = dot(ahead(base, 81 * j)[:, :128].astype(BF), k["up_mid"][...]).astype(BF)
        rows = jnp.concatenate([spread[:, 128 * q : 128 * q + 128] for q in range(4)], axis=0)
        risen = dot(s["wxm"][...], rows)
        for a in range(2):
            lanes = slice((2 * j + a) * 128, (2 * j + a + 1) * 128)
            total = risen[64 * a : 64 * a + 64] + full_e1[:, lanes].astype(F32)
            full_m[:, lanes] = total.astype(BF)
    conv(MID, full_m, s["wm"].at[2], mid_m)
    conv(MID, mid_m, s["wm"].at[3], s["f1"])
    raw_f1 = s["raw_f1"]
    keep_inside(MID, s["f1"], raw_f1)
    pack(MID, raw_f1, box_of("msg_f1"))
    sent_f1 = exchange(MID, raw_f1, box_of("msg_f1"), box_of("got_f1"), s["ss"].at[5], s["rs"].at[5])

    full_e0 = s["full_e0"]
    unpack(FINE, raw_e0, box_of("got_e0"), full_e0, sent_e0)
    unpack(MID, raw_f1, box_of("got_f1"), s["full_f1"], sent_f1)
    for j in range(8):
        spread = dot(s["full_f1"][:, (j + 1) * 128 : (j + 2) * 128], k["up_fine"][...]).astype(BF)
        rows = jnp.concatenate([spread[:, 256 * q : 256 * q + 256] for q in range(4)], axis=0)
        risen = dot(s["wx"][...], rows)
        for a in range(2):
            lanes = slice((2 * j + a) * 256, (2 * j + a + 1) * 256)
            total = risen[32 * a : 32 * a + 32] + full_e0[:, lanes].astype(F32)
            full_x[:, lanes] = total.astype(BF)
    conv(FINE, full_x, s["wf"].at[2], mid_f)
    conv(FINE, mid_f, s["wf"].at[3], s["e0"])
    rows = jnp.concatenate([s["e0"][:, (p + 2) * 256 : (p + 3) * 256] for p in range(12)], axis=0)
    out_ref[...] = dot(rows, k["leave"][...])[:, :144].astype(BF)
    for copy in started:
        copy.wait_send()


def scratch(nyz, place_of):
    nzh, ny, nx = place_of
    fine, mid = (32, 16 * 256), (64, 10 * 128)
    count = 1 + nzh * (ny - 1) + 3 * nzh * ny + nyz
    vm = lambda *shape: pltpu.VMEM(shape, BF)
    return dict(
        raw_x=vm(*fine), full_x=vm(*fine), mid_f=vm(*fine), e0=vm(*fine), raw_e0=vm(*fine), full_e0=vm(*fine),
        raw_h1=vm(*mid), full_m=vm(*mid), mid_m=vm(*mid), e1=vm(*mid), raw_e1=vm(*mid), full_e1=vm(*mid),
        f1=vm(*mid), raw_f1=vm(*mid), full_f1=vm(*mid),
        **{
            f"{way}_{name}_{part}": vm(*shape)
            for way in ("msg", "got")
            for name in ("x", "e0", "h1", "e1", "f1")
            for part, shape in dict(
                face=(8, 3, 32, 128) if name in ("x", "e0") else (8, 1, 64, 128),
                wing=(2, 8, 16, 128),
                corner=(8, 16, 128),
                end=(2, 64, 128),
            ).items()
            if part != "end" or name not in ("x", "e0")
        },
        msg_b=vm(64, 128), got_b=vm(27, 64, 128),
        b0=vm(256, FLAT), b1=vm(256, OUT1), b2=vm(256, OUT2),
        wf=vm(4, 96, 288), wm=vm(4, 192, 576), wr=vm(64, 256), wrm=vm(256, 512), wx=vm(64, 256), wxm=vm(128, 1024),
        gathered=vm(2, 2, 1024, 896), taps=vm(864, 896), blocks=vm(FLAT, FLAT),
        cols_f=vm(288, 1024), cols_m=vm(576, 640), cols_r=vm(256, 1536), cols_rm=vm(512, 384), cols_b=vm(896, OUT1),
        sums_f=pltpu.VMEM((96, 16 * 256), F32), sums_m=pltpu.VMEM((192, 1280), F32), acc=pltpu.VMEM((256, OUT1), F32),
        ss=pltpu.SemaphoreType.DMA((6, 26)), rs=pltpu.SemaphoreType.DMA((6, 26)),
        gs=pltpu.SemaphoreType.DMA((count,)), gr=pltpu.SemaphoreType.DMA((count,)), ps=pltpu.SemaphoreType.DMA((2,)),
    )


SCRATCH = tuple(scratch(64, (2, 8, 4)))


def solution(mesh):
    ngx, nyz = mesh.shape["gx"], mesh.shape["yz"]
    place_of = (2, 8, 4) if nyz == 64 else (1, math.isqrt(nyz), math.isqrt(nyz))
    tables = {name: np.asarray(value, BF) for name, value in constants().items()}

    def body(features_in, *weights):
        planes = features_in[0].transpose(1, 0, 2).reshape(384, 144)
        result = pl.pallas_call(
            lambda *refs: kernel(ngx, nyz, place_of, *refs),
            name="unet",
            out_shape=jax.ShapeDtypeStruct((384, 144), BF),
            in_specs=[pl.BlockSpec(memory_space=pltpu.VMEM)] * (1 + len(NAMES) + len(CONST)),
            out_specs=pl.BlockSpec(memory_space=pltpu.VMEM),
            scratch_shapes=list(scratch(nyz, place_of).values()),
            compiler_params=pltpu.CompilerParams(
                collective_id=0, has_side_effects=True, vmem_limit_bytes=60 * 2**20
            ),
        )(planes, *weights, *(jnp.asarray(tables[name]) for name in CONST))
        return result.reshape(12, 32, 144).transpose(1, 0, 2)[None]

    placed = tuple(
        P("yz", None, "gx", None) if i == 0 else P("yz", None) if i in (7, 8) else P() for i in range(15)
    )
    return jax.shard_map(
        body, mesh=mesh, in_specs=placed, out_specs=P("yz", None, "gx", None), check_vma=False
    )
```

```python
import math

import jax
import jax.numpy as jnp
import numpy as np
from jax import lax
from jax.experimental import pallas as pl
from jax.experimental.pallas import tpu as pltpu
from jax.sharding import PartitionSpec as P

MESH = pl.DeviceIdType.MESH
BF = jnp.bfloat16
F32 = jnp.float32
YZ8 = [(b, c) for b in (-1, 0, 1) for c in (-1, 0, 1) if (b, c) != (0, 0)]
ALL26 = [
    (a, b, c)
    for a in (-1, 0, 1)
    for b in (-1, 0, 1)
    for c in (-1, 0, 1)
    if (a, b, c) != (0, 0, 0)
]


CORNERS = [d for d, (b, c) in enumerate(YZ8) if b and c]


class Level:
    def __init__(self, width, extent, stride, lanes, group):
        self.width, self.extent, self.stride, self.lanes = width, extent, stride, lanes
        self.planes = extent + 4
        self.share = lanes // 8
        self.per_tile = 128 // self.share
        self.tiles = -(-extent // self.per_tile)
        self.group = group
        self.fold = width // 16
        self.span = 128 // self.fold

    def lane(self, y, z):
        return (y + 2) * self.stride + z + 2

    def region(self, step):
        e = self.extent
        return {-1: (0, 1), 0: tuple(range(e)), 1: (e - 2, e - 1)}[step]

    def tables(self):
        pack = np.zeros((self.lanes, self.lanes), np.float32)
        unpack = np.zeros((self.lanes, self.lanes), np.float32)
        for d, (b, c) in enumerate(YZ8):
            cell = 0
            for y in self.region(b):
                for z in self.region(c):
                    slot = d * self.share + cell
                    pack[self.lane(y, z), slot] = 1
                    unpack[slot, self.lane(y - self.extent * b, z - self.extent * c)] = 1
                    cell += 1
        return pack, unpack


FINE = Level(32, 12, 16, 256, 4)
MID = Level(64, 6, 10, 128, 5)
FLAT = 896
OUT1, OUT2 = 640, 384


def constants():
    place = np.zeros((144, 256), np.float32)
    for y in range(12):
        for z in range(12):
            place[y * 12 + z, FINE.lane(y, z)] = 1
    eight = np.zeros((256, 256), np.float32)
    for i in range(32):
        for t in range(8):
            eight[8 * i + t, 32 * t + i] = 1
    down = np.zeros((256, 128), np.float32)
    for y in range(6):
        for z in range(6):
            down[FINE.lane(2 * y, 2 * z), MID.lane(y, z)] = 1
    down_bottom = np.zeros((384, 128), np.float32)
    for j in range(3):
        for y in range(3):
            for z in range(3):
                down_bottom[128 * j + MID.lane(2 * y, 2 * z), 9 * j + 3 * y + z] = 1
    up_fine = np.zeros((128, 1024), np.float32)
    for y in range(16):
        for z in range(16):
            part = 2 * (y % 2) + z % 2
            up_fine[(y // 2 + 1) * 10 + z // 2 + 1, 256 * part + 16 * y + z] = 1
    up_mid = np.zeros((128, 512), np.float32)
    for y in range(10):
        for z in range(10):
            part = 2 * (y % 2) + z % 2
            up_mid[9 * (y // 2) + z // 2, 128 * part + 10 * y + z] = 1
    pick = []
    for width in (32, 64):
        table = np.zeros((2 * width, 8 * width), np.float32)
        for a in range(2):
            for o in range(width):
                for part in range(4):
                    table[a * width + o, 8 * o + 4 * a + part] = 1
        pick.append(table)
    fine_pack, fine_unpack = FINE.tables()
    mid_pack, mid_unpack = MID.tables()
    return dict(
        place=place,
        leave=np.pad(place.T, ((0, 0), (0, 112))),
        eight=eight,
        down=down,
        down_bottom=down_bottom,
        up_fine=up_fine,
        up_mid=up_mid,
        pick_fine=pick[0],
        pick_mid=pick[1],
        fine_pack=fine_pack,
        fine_unpack=fine_unpack,
        mid_pack=mid_pack,
        mid_unpack=mid_unpack,
    )


NAMES = (
    "efa", "efb", "rf", "ema", "emb", "rm", "ba", "bb", "xm", "dma", "dmb", "xf", "dfa", "dfb",
)
CONST = tuple(constants().keys())


def ahead(value, shift):
    width = value.shape[1]
    shift = -shift % width
    return value if shift == 0 else pltpu.roll(value, shift, 1)


def dot(a, b):
    return jnp.dot(a, b, preferred_element_type=F32)


def dot_nt(a, b):
    return lax.dot_general(a, b, (((1,), (1,)), ((), ())), preferred_element_type=F32)


def group_of(rows, size):
    return lax.broadcasted_iota(jnp.int32, (rows, 128), 1) // size


def kernel(ngx, nyz, place_of, x_ref, *refs):
    w = dict(zip(NAMES, refs[: len(NAMES)]))
    refs = refs[len(NAMES) :]
    k = dict(zip(CONST, refs[: len(CONST)]))
    refs = refs[len(CONST) :]
    out_ref = refs[0]
    s = dict(zip(SCRATCH, refs[1:]))
    across = math.isqrt(nyz)
    nzh, ny, nx = place_of
    gx, yz = lax.axis_index("gx"), lax.axis_index("yz")

    def device(a, b, c):
        row, col = yz // across, yz % across
        return (
            (gx + a + ngx) % ngx,
            (row + b + across) % across * across + (col + c + across) % across,
        )

    zh, gy, gxx = yz // (ny * nx), yz // nx % ny, yz % nx
    core = gx % 2
    partner = (gx + 1 - 2 * core, yz)
    rs = 1024 // nyz

    def at(z, y, x):
        return z * ny * nx + y * nx + x

    z_peer = ((ngx // 2 - 1 - gx // 2) * 2 + core, at(1 - zh, gy, gxx))
    y_next = (gx, at(zh, (gy + 1) % ny, gxx))
    y_last = (gx, at(zh, (gy + ny - 1) % ny, gxx))
    x_next = (gx, at(zh, gy, (gxx + 1) % nx))
    x_last = (gx, at(zh, gy, (gxx + nx - 1) % nx))

    barrier = pltpu.get_barrier_semaphore()
    greet = [device(*d) for d in ALL26] + [y_next, y_last, x_next, x_last, partner]
    if nzh == 2:
        greet.append(z_peer)
    for peer in greet:
        pl.semaphore_signal(barrier, inc=1, device_id=peer, device_id_type=MESH)

    def box_of(name):
        return {part: s[name + "_" + part] for part in ("face", "wing", "corner", "end") if name + "_" + part in s}

    started = []

    def send(src, dst, ssem, rsem, peer):
        copy = pltpu.make_async_remote_copy(
            src_ref=src, dst_ref=dst, send_sem=ssem, recv_sem=rsem, device_id=peer, device_id_type=MESH
        )
        copy.start()
        started.append(copy)
        return copy

    for level, ref in ((FINE, s["mid_f"]), (MID, s["mid_m"])):
        n, last = level.lanes, (level.planes - 1) * level.lanes
        ref[:, 0:n] = jnp.zeros((level.width, n), BF)
        ref[:, last : last + n] = jnp.zeros((level.width, n), BF)

    raw_x = s["raw_x"]
    planes = dot(x_ref[...], k["place"][...]).astype(BF)
    for p in range(12):
        raw_x[:, (p + 2) * 256 : (p + 3) * 256] = planes[32 * p : 32 * p + 32]

    def folded(level, value, start):
        which = group_of(16, level.span)
        tile = jnp.zeros((16, 128), BF)
        for h in range(level.fold):
            tile = jnp.where(which == h, ahead(value[16 * h : 16 * h + 16], start - level.span * h), tile)
        return tile

    def unfolded(level, value, start):
        return jnp.concatenate([ahead(value, level.span * h - start) for h in range(level.fold)], axis=0)

    def pack(level, raw, box):
        c, e, n = level.width, level.extent, level.lanes
        table = k["fine_pack" if level is FINE else "mid_pack"]
        which = group_of(c, level.share)
        which4 = group_of(c, 4)
        corners = [jnp.zeros((c, 128), BF)] * 8
        for t in range(level.tiles):
            members = range(t * level.per_tile, min(e, (t + 1) * level.per_tile))
            rows = jnp.concatenate([raw[:, (p + 2) * n : (p + 3) * n] for p in members], axis=0)
            faces = dot(rows, table[...]).astype(BF)
            for d in range(8):
                half, base = divmod(d * level.share, 128)
                tile = jnp.zeros((c, 128), BF)
                for q, p in enumerate(members):
                    part = faces[q * c : (q + 1) * c, 128 * half : 128 * half + 128]
                    tile = jnp.where(which == q, ahead(part, base - q * level.share), tile)
                    if d in CORNERS:
                        corners[d] = jnp.where(which4 == p, ahead(part, base - 4 * p), corners[d])
                if d not in CORNERS:
                    box["face"][d, t] = tile
                if t == level.tiles - 1:
                    box["wing"][1, d] = folded(level, tile, 64)
                if t == 0:
                    box["wing"][0, d] = folded(level, tile, 0)
        for d in CORNERS:
            box["corner"][d] = folded(level, corners[d], 0)
        if level is MID:
            low = lax.broadcasted_iota(jnp.int32, (c, 128), 1) < 64
            for side, first in ((1, e), (0, 2)):
                a = raw[:, first * n : (first + 1) * n]
                b = raw[:, (first + 1) * n : (first + 2) * n]
                box["end"][side] = jnp.where(low, ahead(a, 22), ahead(b, 22 - 64))

    def exchange(level, raw, box, got, ssem, rsem):
        n, e = level.lanes, level.extent
        copies = []
        for m, (a, b, c) in enumerate(ALL26):
            side = 1 if a == 1 else 0
            if (b, c) == (0, 0):
                if level is MID:
                    src, dst = box["end"].at[side], got["end"].at[side]
                elif a == 1:
                    src, dst = raw.at[:, e * n : (e + 2) * n], raw.at[:, 0 : 2 * n]
                else:
                    src, dst = raw.at[:, 2 * n : 4 * n], raw.at[:, (e + 2) * n : (e + 4) * n]
            else:
                d = YZ8.index((b, c))
                if a != 0:
                    src, dst = box["wing"].at[side, d], got["wing"].at[side, d]
                elif d in CORNERS:
                    src, dst = box["corner"].at[d], got["corner"].at[d]
                else:
                    src, dst = box["face"].at[d], got["face"].at[d]
            copies.append(send(src, dst, ssem.at[m], rsem.at[m], device(a, b, c)))
        return copies

    def unpack(level, raw, got, full, copies):
        c, e, n = level.width, level.extent, level.lanes
        table = k["fine_unpack" if level is FINE else "mid_unpack"]
        which = group_of(c, level.share)
        for copy in copies:
            copy.wait_recv()
        if level is MID:
            lane = lax.broadcasted_iota(jnp.int32, (c, 128), 1)
            mine = (lane >= 22) & (lane < 86)
            zero = jnp.zeros((c, 128), BF)
            for side, first in ((1, 0), (0, e + 2)):
                value = got["end"][side]
                for q in range(2):
                    lanes = slice((first + q) * n, (first + q + 1) * n)
                    raw[:, lanes] = jnp.where(mine, ahead(value, 64 * q - 22), zero)
        corner = {d: unfolded(level, got["corner"][d], 0) for d in CORNERS}
        wing = {
            (side, d): unfolded(level, got["wing"][side, d], 64 * side) for side in range(2) for d in range(8)
        }

        def halo(plane):
            p = plane - 2
            halves = []
            for half in range(n // 128):
                value = jnp.zeros((c, 128), BF)
                for d in range(8):
                    if d * level.share // 128 != half:
                        continue
                    base = d * level.share % 128
                    if p < 0:
                        piece, start = wing[1, d], (p + e) % level.per_tile * level.share
                    elif p >= e:
                        piece, start = wing[0, d], (p - e) * level.share
                    elif d in CORNERS:
                        piece, start = corner[d], 4 * p
                    else:
                        piece = got["face"][d, p // level.per_tile]
                        start = p % level.per_tile * level.share
                    value = jnp.where(which == base // level.share, ahead(piece, start - base), value)
                halves.append(value)
            return jnp.concatenate(halves, axis=1) if len(halves) > 1 else halves[0]

        step = 4 if level is FINE else 5
        for first in range(0, level.planes, step):
            members = range(first, first + step)
            rows = jnp.concatenate([halo(m) for m in members], axis=0)
            placed = dot(rows, table[...]).astype(BF)
            for q, m in enumerate(members):
                own = raw[:, m * n : (m + 1) * n]
                full[:, m * n : (m + 1) * n] = own + placed[q * c : (q + 1) * c]

    def conv(level, src, weight, dst):
        c, n = level.width, level.lanes
        width = level.group * n
        cols, sums = (s["cols_f"], s["sums_f"]) if level is FINE else (s["cols_m"], s["sums_m"])

        def one(g, carry):
            lanes = pl.ds(pl.multiple_of(g * width, width), width)
            for ib in range(c // 32):
                rows = src[32 * ib : 32 * ib + 32, lanes]
                for t in range(9):
                    shift = level.stride * (t // 3 - 1) + t % 3 - 1
                    top = 288 * ib + 32 * t
                    cols[top : top + 32, :] = ahead(rows, shift)
            sums[:, lanes] = dot(weight[...], cols[...])
            return carry

        lax.fori_loop(0, level.planes // level.group, one, 0)

        def two(x, carry):
            def lanes(d):
                return pl.ds(pl.multiple_of((x + d) * n, n), n)

            total = sums[0:c, lanes(-1)] + sums[c : 2 * c, lanes(0)] + sums[2 * c : 3 * c, lanes(1)]
            dst[:, lanes(0)] = jnp.maximum(total, 0.0).astype(BF)
            return carry

        lax.fori_loop(1, level.planes - 1, two, 0)

    taps = s["taps"]
    column = lax.broadcasted_iota(jnp.int32, (1, 896), 1)
    wanted = jnp.where(column < 864, 27 * (column & 31) + (column >> 5), -1)
    row = lax.broadcasted_iota(jnp.int32, (32, 896), 0)

    def tap_rows(n, carry):
        taps[pl.ds(pl.multiple_of(n * 32, 32), 32), :] = jnp.where(row + 32 * n == wanted, 1.0, 0.0).astype(BF)
        return carry

    lax.fori_loop(0, 27, tap_rows, 0)
    g_ref = s["gathered"]
    own_rows = pl.ds(pl.multiple_of(yz * rs, rs), rs)
    for m, name in enumerate(("ba", "bb")):
        for ib in range(2):
            part = w[name][:, 864 * ib : 864 * ib + 864]
            g_ref[m, ib, own_rows, :] = dot(part, taps[...]).astype(BF)

    pack(FINE, raw_x, box_of("msg_x"))
    pl.semaphore_wait(barrier, len(greet))
    sent_x = exchange(FINE, raw_x, box_of("msg_x"), box_of("got_x"), s["ss"].at[0], s["rs"].at[0])

    def piece(ref, j):
        return ref.at[core, :, pl.ds(pl.multiple_of(j * rs, rs), rs), :]

    nsend = [0]
    waiting = {}

    def pass_on(j, key, peer):
        n = nsend[0]
        nsend[0] += 1
        waiting[key] = send(piece(g_ref, j), piece(g_ref, j), s["gs"].at[n], s["gr"].at[n], peer)

    zs = [zh, 1 - zh] if nzh == 2 else [zh]

    up, down = ny // 2, (ny - 1) // 2

    def along_y(i, n):
        if n < up:
            pass_on(at(zs[i], (gy - n + ny) % ny, gxx), ("y+", i, n + 1), y_next)
        if n < down:
            pass_on(at(zs[i], (gy + n) % ny, gxx), ("y-", i, n + 1), y_last)

    def along_x(i, d, local):
        j = at(zs[i], (gy - d + ny) % ny, gxx)
        pass_on(j, ("x+", i, d), x_next)
        if nx > 2:
            pass_on(j, ("x-", i, d), x_last)
        if not local:
            pass_on(j, ("p", i, d, 0), partner)

    if nzh == 2:
        pass_on(yz, "z", z_peer)
    along_y(0, 0)
    along_x(0, 0, True)

    for n, name in enumerate(("efa", "efb", "dfa", "dfb")):
        flat = dot(w[name][...], taps[...])
        for a in range(3):
            s["wf"][n, 32 * a : 32 * a + 32, :] = ahead(flat, 288 * a)[:, :288].astype(BF)
    lane = lax.broadcasted_iota(jnp.int32, (64, 896), 1)
    for n, name in enumerate(("ema", "emb", "dma", "dmb")):
        low = dot(w[name][:, 0:864], taps[...])
        high = dot(w[name][:, 864:1728], taps[...])
        for a in range(3):
            both = jnp.where(lane < 288, ahead(low, 288 * a), ahead(high, 288 * a - 288))
            s["wm"][n, 64 * a : 64 * a + 64, :] = both[:, :576].astype(BF)
    s["wr"][...] = dot(w["rf"][...], k["eight"][...]).astype(BF)
    for ib in range(2):
        s["wrm"][:, 256 * ib : 256 * ib + 256] = dot(
            w["rm"][:, 256 * ib : 256 * ib + 256], k["eight"][...]
        ).astype(BF)
    for name, table, into, wide in (("xf", "pick_fine", "wx", 256), ("xm", "pick_mid", "wxm", 512)):
        value = w[name][...].astype(F32)
        part = lax.broadcasted_iota(jnp.int32, value.shape, 1) % 4
        rows = jnp.concatenate([jnp.where(part == q, value, 0.0) for q in range(4)], axis=0)
        s[into][...] = dot_nt(k[table][...], rows.astype(BF)).astype(BF)

    column = lax.broadcasted_iota(jnp.int32, (32, FLAT), 1)
    cell = lax.broadcasted_iota(jnp.int32, (32, 1), 0)
    cx = (cell * 57) >> 9
    cy = ((cell - 9 * cx) * 11) >> 5
    offset = jnp.where(cell < 27, 72 * cx + 6 * cy + cell, -4096)
    blocks = s["blocks"]
    blocks[864:896, :] = jnp.zeros((32, FLAT), BF)

    def block_rows(b, carry):
        first = 81 * 3 * (2 - b // 9) + 9 * 3 * (2 - b // 3 % 3) + 3 * (2 - b % 3)
        blocks[pl.ds(pl.multiple_of(b * 32, 32), 32), :] = jnp.where(column == offset + first, 1.0, 0.0).astype(BF)
        return carry

    lax.fori_loop(0, 27, block_rows, 0)

    def step_y(i, n):
        if i < nzh and n <= up:
            waiting["y+", i, n].wait_recv()
            if n <= down:
                waiting["y-", i, n].wait_recv()
            along_y(i, n)
            along_x(i, n, False)
            if n <= down:
                along_x(i, ny - n, False)

    if nzh == 2:
        waiting["z"].wait_recv()
        along_y(1, 0)
        along_x(1, 0, False)

    full_x, mid_f = s["full_x"], s["mid_f"]
    for n, i in ((1, 0), (1, 1), (2, 0), (2, 1)):
        step_y(i, n)
    unpack(FINE, raw_x, box_of("got_x"), full_x, sent_x)
    conv(FINE, full_x, s["wf"].at[0], mid_f)
    step_y(0, 3)
    step_y(1, 3)
    raw_e0 = s["raw_e0"]
    conv(FINE, mid_f, s["wf"].at[1], s["e0"])

    def keep_inside(level, src, raw):
        n = level.lanes
        cells = lax.broadcasted_iota(jnp.int32, (1, n), 1)
        y, z = cells // level.stride - 2, cells % level.stride - 2
        inside = (y >= 0) & (y < level.extent) & (z >= 0) & (z < level.extent)
        for p in range(2, level.extent + 2):
            value = src[:, p * n : (p + 1) * n]
            raw[:, p * n : (p + 1) * n] = jnp.where(inside, value, jnp.zeros_like(value))

    keep_inside(FINE, s["e0"], raw_e0)

    own = raw_e0[:, 512 : 14 * 256]
    for t in range(4):
        moved = ahead(own, 16 * (t // 2) + t % 2)
        for j in range(6):
            for a in range(2):
                top = 128 * a + 32 * t
                s["cols_r"][top : top + 32, 256 * j : 256 * j + 256] = moved[
                    :, 256 * (2 * j + a) : 256 * (2 * j + a) + 256
                ]
    wide = dot(s["wr"][...], s["cols_r"][...]).astype(BF)
    rows = jnp.concatenate([wide[:, 256 * j : 256 * j + 256] for j in range(6)], axis=0)
    small = dot(rows, k["down"][...]).astype(BF)
    raw_h1 = s["raw_h1"]
    for j in range(6):
        raw_h1[:, (j + 2) * 128 : (j + 3) * 128] = small[64 * j : 64 * j + 64]
    pack(MID, raw_h1, box_of("msg_h1"))
    sent_h1 = exchange(MID, raw_h1, box_of("msg_h1"), box_of("got_h1"), s["ss"].at[1], s["rs"].at[1])
    for n in range(4, up + 1):
        step_y(0, n)
        step_y(1, n)

    full_m, mid_m = s["full_m"], s["mid_m"]
    unpack(MID, raw_h1, box_of("got_h1"), full_m, sent_h1)
    conv(MID, full_m, s["wm"].at[0], mid_m)
    conv(MID, mid_m, s["wm"].at[1], s["e1"])
    raw_e1 = s["raw_e1"]
    keep_inside(MID, s["e1"], raw_e1)

    own = raw_e1[:, 256 : 8 * 128]
    for t in range(4):
        moved = ahead(own, 10 * (t // 2) + t % 2)
        for j in range(3):
            for a in range(2):
                for ib in range(2):
                    top = 256 * ib + 128 * a + 32 * t
                    s["cols_rm"][top : top + 32, 128 * j : 128 * j + 128] = moved[
                        32 * ib : 32 * ib + 32, 128 * (2 * j + a) : 128 * (2 * j + a) + 128
                    ]
    wide = dot(s["wrm"][...], s["cols_rm"][...]).astype(BF)
    cells = dot(wide, k["down_bottom"][...]).astype(BF)
    which = group_of(64, 32)
    tile = jnp.zeros((64, 128), BF)
    for q in range(4):
        tile = jnp.where(which == q, ahead(cells[64 * q : 64 * q + 64], -32 * q), tile)
    s["msg_b"][...] = tile
    got_b = s["got_b"]
    got_b[13] = tile
    sent_b = []
    for m, (a, b, c) in enumerate(ALL26):
        slot = 9 * (a + 1) + 3 * (b + 1) + c + 1
        sent_b.append(
            send(s["msg_b"], got_b.at[slot], s["ss"].at[3, m], s["rs"].at[3, m], device(a, b, c))
        )
    pack(MID, raw_e1, box_of("msg_e1"))
    sent_e1 = exchange(MID, raw_e1, box_of("msg_e1"), box_of("got_e1"), s["ss"].at[4], s["rs"].at[4])

    order = [(i, d) for i in range(nzh) for d in sorted(range(ny), key=lambda d: min(d, ny - d))]
    for i, d in order:
        y = (gy - d + ny) % ny
        waiting["x+", i, d].wait_recv()
        j = at(zs[i], y, (gxx + nx - 1) % nx)
        if nx > 2 and i == 0:
            pass_on(j, ("f", i, d), x_next)
        pass_on(j, ("p", i, d, 1), partner)
        if nx > 2:
            waiting["x-", i, d].wait_recv()
            j = at(zs[i], y, (gxx + 1) % nx)
            if i == 1:
                pass_on(j, ("f", i, d), x_last)
            pass_on(j, ("p", i, d, 2), partner)
    pack(FINE, raw_e0, box_of("msg_e0"))
    sent_e0 = exchange(FINE, raw_e0, box_of("msg_e0"), box_of("got_e0"), s["ss"].at[2], s["rs"].at[2])
    if nx > 2:
        for i, d in order:
            waiting["f", i, d].wait_recv()
            pass_on(at(zs[i], (gy - d + ny) % ny, (gxx + 2) % nx), ("p", i, d, 3), partner)

    for copy in sent_b:
        copy.wait_recv()
    for q in range(4):
        tiles = []
        for t in range(7):
            tile = jnp.zeros((64, 128), BF)
            for b in range(4):
                if 4 * t + b < 27:
                    tile = jnp.where(
                        which == b, ahead(got_b[4 * t + b], 32 * (q - b)), tile
                    )
            tiles.append(tile)
        s["b0"][64 * q : 64 * q + 64, :] = dot(jnp.concatenate(tiles, axis=1), blocks[...]).astype(BF)
    for key, copy in waiting.items():
        if key[0] == "p":
            copy.wait_recv()
    cols_b, acc = s["cols_b"], s["acc"]
    cols_b[864:896, :] = jnp.zeros((32, OUT1), BF)

    def bottom(src, m, dst, width):
        acc[:, :width] = jnp.zeros((256, width), F32)

        def one(kk, carry):
            rows = src[pl.ds(pl.multiple_of(kk * 32, 32), 32), :]
            for t in range(27):
                shift = 81 * (t // 9) + 9 * (t // 3 % 3) + t % 3
                cols_b[32 * t : 32 * t + 32, :width] = ahead(rows, shift)[:, :width]
            lhs = g_ref[m, kk % 2, pl.ds(pl.multiple_of(kk // 2 * 256, 256), 256), :]
            acc[:, :width] += dot(lhs, cols_b[:, :width])
            return carry

        lax.fori_loop(0, 8, one, 0)
        dst[...] = jnp.maximum(acc[:, :width], 0.0).astype(BF)

    bottom(s["b0"], 0, s["b1"], OUT1)
    bottom(s["b1"], 1, s["b2"], OUT2)

    full_e1 = s["full_e1"]
    unpack(MID, raw_e1, box_of("got_e1"), full_e1, sent_e1)
    base = s["b2"][...]
    for j in range(5):
        spread = dot(ahead(base, 81 * j)[:, :128], k["up_mid"][...]).astype(BF)
        rows = jnp.concatenate([spread[:, 128 * q : 128 * q + 128] for q in range(4)], axis=0)
        risen = dot(s["wxm"][...], rows)
        for a in range(2):
            lanes = slice((2 * j + a) * 128, (2 * j + a + 1) * 128)
            total = risen[64 * a : 64 * a + 64] + full_e1[:, lanes].astype(F32)
            full_m[:, lanes] = total.astype(BF)
    conv(MID, full_m, s["wm"].at[2], mid_m)
    conv(MID, mid_m, s["wm"].at[3], s["f1"])
    raw_f1 = s["raw_f1"]
    keep_inside(MID, s["f1"], raw_f1)
    pack(MID, raw_f1, box_of("msg_f1"))
    sent_f1 = exchange(MID, raw_f1, box_of("msg_f1"), box_of("got_f1"), s["ss"].at[5], s["rs"].at[5])

    full_e0 = s["full_e0"]
    unpack(FINE, raw_e0, box_of("got_e0"), full_e0, sent_e0)
    unpack(MID, raw_f1, box_of("got_f1"), s["full_f1"], sent_f1)
    for j in range(8):
        spread = dot(s["full_f1"][:, (j + 1) * 128 : (j + 2) * 128], k["up_fine"][...]).astype(BF)
        rows = jnp.concatenate([spread[:, 256 * q : 256 * q + 256] for q in range(4)], axis=0)
        risen = dot(s["wx"][...], rows)
        for a in range(2):
            lanes = slice((2 * j + a) * 256, (2 * j + a + 1) * 256)
            total = risen[32 * a : 32 * a + 32] + full_e0[:, lanes].astype(F32)
            full_x[:, lanes] = total.astype(BF)
    conv(FINE, full_x, s["wf"].at[2], mid_f)
    conv(FINE, mid_f, s["wf"].at[3], s["e0"])
    rows = jnp.concatenate([s["e0"][:, (p + 2) * 256 : (p + 3) * 256] for p in range(12)], axis=0)
    out_ref[...] = dot(rows, k["leave"][...])[:, :144].astype(BF)
    for copy in started:
        copy.wait_send()


def scratch(nyz, place_of):
    nzh, ny, nx = place_of
    fine, mid = (32, 16 * 256), (64, 10 * 128)
    count = 1 + nzh * (ny - 1) + 3 * nzh * ny + nyz
    vm = lambda *shape: pltpu.VMEM(shape, BF)
    return dict(
        raw_x=vm(*fine), full_x=vm(*fine), mid_f=vm(*fine), e0=vm(*fine), raw_e0=vm(*fine), full_e0=vm(*fine),
        raw_h1=vm(*mid), full_m=vm(*mid), mid_m=vm(*mid), e1=vm(*mid), raw_e1=vm(*mid), full_e1=vm(*mid),
        f1=vm(*mid), raw_f1=vm(*mid), full_f1=vm(*mid),
        **{
            f"{way}_{name}_{part}": vm(*shape)
            for way in ("msg", "got")
            for name in ("x", "e0", "h1", "e1", "f1")
            for part, shape in dict(
                face=(8, 3, 32, 128) if name in ("x", "e0") else (8, 1, 64, 128),
                wing=(2, 8, 16, 128),
                corner=(8, 16, 128),
                end=(2, 64, 128),
            ).items()
            if part != "end" or name not in ("x", "e0")
        },
        msg_b=vm(64, 128), got_b=vm(27, 64, 128),
        b0=vm(256, FLAT), b1=vm(256, OUT1), b2=vm(256, OUT2),
        wf=vm(4, 96, 288), wm=vm(4, 192, 576), wr=vm(64, 256), wrm=vm(256, 512), wx=vm(64, 256), wxm=vm(128, 1024),
        gathered=vm(2, 2, 1024, 896), taps=vm(864, 896), blocks=vm(FLAT, FLAT),
        cols_f=vm(288, 1024), cols_m=vm(576, 640), cols_r=vm(256, 1536), cols_rm=vm(512, 384), cols_b=vm(896, OUT1),
        sums_f=pltpu.VMEM((96, 16 * 256), F32), sums_m=pltpu.VMEM((192, 1280), F32), acc=pltpu.VMEM((256, OUT1), F32),
        ss=pltpu.SemaphoreType.DMA((6, 26)), rs=pltpu.SemaphoreType.DMA((6, 26)),
        gs=pltpu.SemaphoreType.DMA((count,)), gr=pltpu.SemaphoreType.DMA((count,)), ps=pltpu.SemaphoreType.DMA((2,)),
    )


SCRATCH = tuple(scratch(64, (2, 8, 4)))


def solution(mesh):
    ngx, nyz = mesh.shape["gx"], mesh.shape["yz"]
    place_of = (2, 8, 4) if nyz == 64 else (1, math.isqrt(nyz), math.isqrt(nyz))
    tables = {name: np.asarray(value, BF) for name, value in constants().items()}

    def body(features_in, *weights):
        planes = features_in[0].transpose(1, 0, 2).reshape(384, 144)
        result = pl.pallas_call(
            lambda *refs: kernel(ngx, nyz, place_of, *refs),
            name="unet",
            out_shape=jax.ShapeDtypeStruct((384, 144), BF),
            in_specs=[pl.BlockSpec(memory_space=pltpu.VMEM)] * (1 + len(NAMES) + len(CONST)),
            out_specs=pl.BlockSpec(memory_space=pltpu.VMEM),
            scratch_shapes=list(scratch(nyz, place_of).values()),
            compiler_params=pltpu.CompilerParams(
                collective_id=0, has_side_effects=True, vmem_limit_bytes=60 * 2**20
            ),
        )(planes, *weights, *(jnp.asarray(tables[name]) for name in CONST))
        return result.reshape(12, 32, 144).transpose(1, 0, 2)[None]

    placed = tuple(
        P("yz", None, "gx", None) if i == 0 else P("yz", None) if i in (7, 8) else P() for i in range(15)
    )
    return jax.shard_map(
        body, mesh=mesh, in_specs=placed, out_specs=P("yz", None, "gx", None), check_vma=False
    )
```

```python
import math

import jax
import jax.numpy as jnp
import numpy as np
from jax import lax
from jax.experimental import pallas as pl
from jax.experimental.pallas import tpu as pltpu
from jax.sharding import PartitionSpec as P

MESH = pl.DeviceIdType.MESH
BF = jnp.bfloat16
F32 = jnp.float32
YZ8 = [(b, c) for b in (-1, 0, 1) for c in (-1, 0, 1) if (b, c) != (0, 0)]
ALL26 = [
    (a, b, c)
    for a in (-1, 0, 1)
    for b in (-1, 0, 1)
    for c in (-1, 0, 1)
    if (a, b, c) != (0, 0, 0)
]


CORNERS = [d for d, (b, c) in enumerate(YZ8) if b and c]


class Level:
    def __init__(self, width, extent, stride, lanes, group):
        self.width, self.extent, self.stride, self.lanes = width, extent, stride, lanes
        self.planes = extent + 4
        self.share = lanes // 8
        self.per_tile = 128 // self.share
        self.tiles = -(-extent // self.per_tile)
        self.group = group
        self.fold = width // 16
        self.span = 128 // self.fold

    def lane(self, y, z):
        return (y + 2) * self.stride + z + 2

    def region(self, step):
        e = self.extent
        return {-1: (0, 1), 0: tuple(range(e)), 1: (e - 2, e - 1)}[step]

    def tables(self):
        pack = np.zeros((self.lanes, self.lanes), np.float32)
        unpack = np.zeros((self.lanes, self.lanes), np.float32)
        for d, (b, c) in enumerate(YZ8):
            cell = 0
            for y in self.region(b):
                for z in self.region(c):
                    slot = d * self.share + cell
                    pack[self.lane(y, z), slot] = 1
                    unpack[slot, self.lane(y - self.extent * b, z - self.extent * c)] = 1
                    cell += 1
        return pack, unpack


FINE = Level(32, 12, 16, 256, 4)
MID = Level(64, 6, 10, 128, 5)
FLAT = 896
OUT1, OUT2 = 640, 384


def constants():
    place = np.zeros((144, 256), np.float32)
    for y in range(12):
        for z in range(12):
            place[y * 12 + z, FINE.lane(y, z)] = 1
    eight = np.zeros((256, 256), np.float32)
    for i in range(32):
        for t in range(8):
            eight[8 * i + t, 32 * t + i] = 1
    down = np.zeros((256, 128), np.float32)
    for y in range(6):
        for z in range(6):
            down[FINE.lane(2 * y, 2 * z), MID.lane(y, z)] = 1
    down_bottom = np.zeros((384, 128), np.float32)
    for j in range(3):
        for y in range(3):
            for z in range(3):
                down_bottom[128 * j + MID.lane(2 * y, 2 * z), 9 * j + 3 * y + z] = 1
    up_fine = np.zeros((128, 1024), np.float32)
    for y in range(16):
        for z in range(16):
            part = 2 * (y % 2) + z % 2
            up_fine[(y // 2 + 1) * 10 + z // 2 + 1, 256 * part + 16 * y + z] = 1
    up_mid = np.zeros((128, 512), np.float32)
    for y in range(10):
        for z in range(10):
            part = 2 * (y % 2) + z % 2
            up_mid[9 * (y // 2) + z // 2, 128 * part + 10 * y + z] = 1
    pick = []
    for width in (32, 64):
        table = np.zeros((2 * width, 8 * width), np.float32)
        for a in range(2):
            for o in range(width):
                for part in range(4):
                    table[a * width + o, 8 * o + 4 * a + part] = 1
        pick.append(table)
    fine_pack, fine_unpack = FINE.tables()
    mid_pack, mid_unpack = MID.tables()
    return dict(
        place=place,
        leave=np.pad(place.T, ((0, 0), (0, 112))),
        eight=eight,
        down=down,
        down_bottom=down_bottom,
        up_fine=up_fine,
        up_mid=up_mid,
        pick_fine=pick[0],
        pick_mid=pick[1],
        fine_pack=fine_pack,
        fine_unpack=fine_unpack,
        mid_pack=mid_pack,
        mid_unpack=mid_unpack,
    )


NAMES = (
    "efa", "efb", "rf", "ema", "emb", "rm", "ba", "bb", "xm", "dma", "dmb", "xf", "dfa", "dfb",
)
CONST = tuple(constants().keys())


def ahead(value, shift):
    width = value.shape[1]
    shift = -shift % width
    return value if shift == 0 else pltpu.roll(value, shift, 1)


def dot(a, b):
    return jnp.dot(a, b, preferred_element_type=F32)


def dot_nt(a, b):
    return lax.dot_general(a, b, (((1,), (1,)), ((), ())), preferred_element_type=F32)


def group_of(rows, size):
    return lax.broadcasted_iota(jnp.int32, (rows, 128), 1) // size


def kernel(ngx, nyz, place_of, x_ref, *refs):
    w = dict(zip(NAMES, refs[: len(NAMES)]))
    refs = refs[len(NAMES) :]
    k = dict(zip(CONST, refs[: len(CONST)]))
    refs = refs[len(CONST) :]
    out_ref = refs[0]
    s = dict(zip(SCRATCH, refs[1:]))
    across = math.isqrt(nyz)
    nzh, ny, nx = place_of
    gx, yz = lax.axis_index("gx"), lax.axis_index("yz")

    def device(a, b, c):
        row, col = yz // across, yz % across
        return (
            (gx + a + ngx) % ngx,
            (row + b + across) % across * across + (col + c + across) % across,
        )

    zh, gy, gxx = yz // (ny * nx), yz // nx % ny, yz % nx
    core = gx % 2
    partner = (gx + 1 - 2 * core, yz)
    rs = 1024 // nyz

    def at(z, y, x):
        return z * ny * nx + y * nx + x

    z_peer = ((ngx // 2 - 1 - gx // 2) * 2 + core, at(1 - zh, gy, gxx))
    y_next = (gx, at(zh, (gy + 1) % ny, gxx))
    y_last = (gx, at(zh, (gy + ny - 1) % ny, gxx))
    x_next = (gx, at(zh, gy, (gxx + 1) % nx))
    x_last = (gx, at(zh, gy, (gxx + nx - 1) % nx))

    barrier = pltpu.get_barrier_semaphore()
    greet = [device(*d) for d in ALL26] + [y_next, y_last, x_next, x_last, partner]
    if nzh == 2:
        greet.append(z_peer)
    for peer in greet:
        pl.semaphore_signal(barrier, inc=1, device_id=peer, device_id_type=MESH)

    def box_of(name):
        return {part: s[name + "_" + part] for part in ("face", "wing", "corner", "end") if name + "_" + part in s}

    started = []

    def send(src, dst, ssem, rsem, peer):
        copy = pltpu.make_async_remote_copy(
            src_ref=src, dst_ref=dst, send_sem=ssem, recv_sem=rsem, device_id=peer, device_id_type=MESH
        )
        copy.start()
        started.append(copy)
        return copy

    for level, ref in ((FINE, s["mid_f"]), (MID, s["mid_m"])):
        n, last = level.lanes, (level.planes - 1) * level.lanes
        ref[:, 0:n] = jnp.zeros((level.width, n), BF)
        ref[:, last : last + n] = jnp.zeros((level.width, n), BF)

    raw_x = s["raw_x"]
    planes = dot(x_ref[...], k["place"][...]).astype(BF)
    for p in range(12):
        raw_x[:, (p + 2) * 256 : (p + 3) * 256] = planes[32 * p : 32 * p + 32]

    def folded(level, value, start):
        which = group_of(16, level.span)
        tile = jnp.zeros((16, 128), BF)
        for h in range(level.fold):
            tile = jnp.where(which == h, ahead(value[16 * h : 16 * h + 16], start - level.span * h), tile)
        return tile

    def unfolded(level, value, start):
        return jnp.concatenate([ahead(value, level.span * h - start) for h in range(level.fold)], axis=0)

    def pack(level, raw, box):
        c, e, n = level.width, level.extent, level.lanes
        table = k["fine_pack" if level is FINE else "mid_pack"]
        which = group_of(c, level.share)
        which4 = group_of(c, 4)
        corners = [jnp.zeros((c, 128), BF)] * 8
        for t in range(level.tiles):
            members = range(t * level.per_tile, min(e, (t + 1) * level.per_tile))
            rows = jnp.concatenate([raw[:, (p + 2) * n : (p + 3) * n] for p in members], axis=0)
            faces = dot(rows, table[...]).astype(BF)
            for d in range(8):
                half, base = divmod(d * level.share, 128)
                tile = jnp.zeros((c, 128), BF)
                for q, p in enumerate(members):
                    part = faces[q * c : (q + 1) * c, 128 * half : 128 * half + 128]
                    tile = jnp.where(which == q, ahead(part, base - q * level.share), tile)
                    if d in CORNERS:
                        corners[d] = jnp.where(which4 == p, ahead(part, base - 4 * p), corners[d])
                if d not in CORNERS:
                    box["face"][d, t] = tile
                if t == level.tiles - 1:
                    box["wing"][1, d] = folded(level, tile, 64)
                if t == 0:
                    box["wing"][0, d] = folded(level, tile, 0)
        for d in CORNERS:
            box["corner"][d] = folded(level, corners[d], 0)
        if level is MID:
            low = lax.broadcasted_iota(jnp.int32, (c, 128), 1) < 64
            for side, first in ((1, e), (0, 2)):
                a = raw[:, first * n : (first + 1) * n]
                b = raw[:, (first + 1) * n : (first + 2) * n]
                box["end"][side] = jnp.where(low, ahead(a, 22), ahead(b, 22 - 64))

    def exchange(level, raw, box, got, ssem, rsem):
        n, e = level.lanes, level.extent
        copies = []
        for m, (a, b, c) in enumerate(ALL26):
            side = 1 if a == 1 else 0
            if (b, c) == (0, 0):
                if level is MID:
                    src, dst = box["end"].at[side], got["end"].at[side]
                elif a == 1:
                    src, dst = raw.at[:, e * n : (e + 2) * n], raw.at[:, 0 : 2 * n]
                else:
                    src, dst = raw.at[:, 2 * n : 4 * n], raw.at[:, (e + 2) * n : (e + 4) * n]
            else:
                d = YZ8.index((b, c))
                if a != 0:
                    src, dst = box["wing"].at[side, d], got["wing"].at[side, d]
                elif d in CORNERS:
                    src, dst = box["corner"].at[d], got["corner"].at[d]
                else:
                    src, dst = box["face"].at[d], got["face"].at[d]
            copies.append(send(src, dst, ssem.at[m], rsem.at[m], device(a, b, c)))
        return copies

    def unpack(level, raw, got, full, copies):
        c, e, n = level.width, level.extent, level.lanes
        table = k["fine_unpack" if level is FINE else "mid_unpack"]
        which = group_of(c, level.share)
        for copy in copies:
            copy.wait_recv()
        if level is MID:
            lane = lax.broadcasted_iota(jnp.int32, (c, 128), 1)
            mine = (lane >= 22) & (lane < 86)
            zero = jnp.zeros((c, 128), BF)
            for side, first in ((1, 0), (0, e + 2)):
                value = got["end"][side]
                for q in range(2):
                    lanes = slice((first + q) * n, (first + q + 1) * n)
                    raw[:, lanes] = jnp.where(mine, ahead(value, 64 * q - 22), zero)
        corner = {d: unfolded(level, got["corner"][d], 0) for d in CORNERS}
        wing = {
            (side, d): unfolded(level, got["wing"][side, d], 64 * side) for side in range(2) for d in range(8)
        }

        def halo(plane):
            p = plane - 2
            halves = []
            for half in range(n // 128):
                value = jnp.zeros((c, 128), BF)
                for d in range(8):
                    if d * level.share // 128 != half:
                        continue
                    base = d * level.share % 128
                    if p < 0:
                        piece, start = wing[1, d], (p + e) % level.per_tile * level.share
                    elif p >= e:
                        piece, start = wing[0, d], (p - e) * level.share
                    elif d in CORNERS:
                        piece, start = corner[d], 4 * p
                    else:
                        piece = got["face"][d, p // level.per_tile]
                        start = p % level.per_tile * level.share
                    value = jnp.where(which == base // level.share, ahead(piece, start - base), value)
                halves.append(value)
            return jnp.concatenate(halves, axis=1) if len(halves) > 1 else halves[0]

        step = 4 if level is FINE else 5
        for first in range(0, level.planes, step):
            members = range(first, first + step)
            rows = jnp.concatenate([halo(m) for m in members], axis=0)
            placed = dot(rows, table[...]).astype(BF)
            for q, m in enumerate(members):
                own = raw[:, m * n : (m + 1) * n]
                full[:, m * n : (m + 1) * n] = own + placed[q * c : (q + 1) * c]

    def conv(level, src, weight, dst):
        c, n = level.width, level.lanes
        width = level.group * n
        cols, sums = (s["cols_f"], s["sums_f"]) if level is FINE else (s["cols_m"], s["sums_m"])

        def one(g, carry):
            lanes = pl.ds(pl.multiple_of(g * width, width), width)
            for ib in range(c // 32):
                rows = src[32 * ib : 32 * ib + 32, lanes]
                for t in range(9):
                    shift = level.stride * (t // 3 - 1) + t % 3 - 1
                    top = 288 * ib + 32 * t
                    cols[top : top + 32, :] = ahead(rows, shift)
            sums[:, lanes] = dot(weight[...], cols[...])
            return carry

        lax.fori_loop(0, level.planes // level.group, one, 0)

        def two(x, carry):
            def lanes(d):
                return pl.ds(pl.multiple_of((x + d) * n, n), n)

            total = sums[0:c, lanes(-1)] + sums[c : 2 * c, lanes(0)] + sums[2 * c : 3 * c, lanes(1)]
            dst[:, lanes(0)] = jnp.maximum(total, 0.0).astype(BF)
            return carry

        lax.fori_loop(1, level.planes - 1, two, 0)

    taps = s["taps"]
    column = lax.broadcasted_iota(jnp.int32, (1, 896), 1)
    wanted = jnp.where(column < 864, 27 * (column & 31) + (column >> 5), -1)
    row = lax.broadcasted_iota(jnp.int32, (32, 896), 0)

    def tap_rows(n, carry):
        taps[pl.ds(pl.multiple_of(n * 32, 32), 32), :] = jnp.where(row + 32 * n == wanted, 1.0, 0.0).astype(BF)
        return carry

    lax.fori_loop(0, 27, tap_rows, 0)
    g_ref = s["gathered"]
    own_rows = pl.ds(pl.multiple_of(yz * rs, rs), rs)
    for m, name in enumerate(("ba", "bb")):
        for ib in range(2):
            part = w[name][:, 864 * ib : 864 * ib + 864]
            g_ref[m, ib, own_rows, :] = dot(part, taps[...]).astype(BF)

    pack(FINE, raw_x, box_of("msg_x"))
    pl.semaphore_wait(barrier, len(greet))
    sent_x = exchange(FINE, raw_x, box_of("msg_x"), box_of("got_x"), s["ss"].at[0], s["rs"].at[0])

    def piece(ref, j):
        return ref.at[core, :, pl.ds(pl.multiple_of(j * rs, rs), rs), :]

    nsend = [0]
    waiting = {}

    def pass_on(j, key, peer):
        n = nsend[0]
        nsend[0] += 1
        waiting[key] = send(piece(g_ref, j), piece(g_ref, j), s["gs"].at[n], s["gr"].at[n], peer)

    zs = [zh, 1 - zh] if nzh == 2 else [zh]

    up, down = ny // 2, (ny - 1) // 2

    def along_y(i, n):
        if n < up:
            pass_on(at(zs[i], (gy - n + ny) % ny, gxx), ("y+", i, n + 1), y_next)
        if n < down:
            pass_on(at(zs[i], (gy + n) % ny, gxx), ("y-", i, n + 1), y_last)

    def along_x(i, d, local):
        j = at(zs[i], (gy - d + ny) % ny, gxx)
        pass_on(j, ("x+", i, d), x_next)
        if nx > 2:
            pass_on(j, ("x-", i, d), x_last)
        if not local:
            pass_on(j, ("p", i, d, 0), partner)

    if nzh == 2:
        pass_on(yz, "z", z_peer)
    along_y(0, 0)
    along_x(0, 0, True)

    for n, name in enumerate(("efa", "efb", "dfa", "dfb")):
        flat = dot(w[name][...], taps[...])
        for a in range(3):
            s["wf"][n, 32 * a : 32 * a + 32, :] = ahead(flat, 288 * a)[:, :288].astype(BF)
    lane = lax.broadcasted_iota(jnp.int32, (64, 896), 1)
    for n, name in enumerate(("ema", "emb", "dma", "dmb")):
        low = dot(w[name][:, 0:864], taps[...])
        high = dot(w[name][:, 864:1728], taps[...])
        for a in range(3):
            both = jnp.where(lane < 288, ahead(low, 288 * a), ahead(high, 288 * a - 288))
            s["wm"][n, 64 * a : 64 * a + 64, :] = both[:, :576].astype(BF)
    s["wr"][...] = dot(w["rf"][...], k["eight"][...]).astype(BF)
    for ib in range(2):
        s["wrm"][:, 256 * ib : 256 * ib + 256] = dot(
            w["rm"][:, 256 * ib : 256 * ib + 256], k["eight"][...]
        ).astype(BF)
    for name, table, into, wide in (("xf", "pick_fine", "wx", 256), ("xm", "pick_mid", "wxm", 512)):
        value = w[name][...].astype(F32)
        part = lax.broadcasted_iota(jnp.int32, value.shape, 1) % 4
        rows = jnp.concatenate([jnp.where(part == q, value, 0.0) for q in range(4)], axis=0)
        s[into][...] = dot_nt(k[table][...], rows.astype(BF)).astype(BF)

    column = lax.broadcasted_iota(jnp.int32, (32, FLAT), 1)
    cell = lax.broadcasted_iota(jnp.int32, (32, 1), 0)
    cx = (cell * 57) >> 9
    cy = ((cell - 9 * cx) * 11) >> 5
    offset = jnp.where(cell < 27, 72 * cx + 6 * cy + cell, -4096)
    blocks = s["blocks"]
    blocks[864:896, :] = jnp.zeros((32, FLAT), BF)

    def block_rows(b, carry):
        first = 81 * 3 * (2 - b // 9) + 9 * 3 * (2 - b // 3 % 3) + 3 * (2 - b % 3)
        blocks[pl.ds(pl.multiple_of(b * 32, 32), 32), :] = jnp.where(column == offset + first, 1.0, 0.0).astype(BF)
        return carry

    lax.fori_loop(0, 27, block_rows, 0)

    def step_y(i, n):
        if i < nzh and n <= up:
            waiting["y+", i, n].wait_recv()
            if n <= down:
                waiting["y-", i, n].wait_recv()
            along_y(i, n)
            along_x(i, n, False)
            if n <= down:
                along_x(i, ny - n, False)

    if nzh == 2:
        waiting["z"].wait_recv()
        along_y(1, 0)
        along_x(1, 0, False)

    full_x, mid_f = s["full_x"], s["mid_f"]
    for n, i in ((1, 0), (1, 1), (2, 0)):
        step_y(i, n)
    unpack(FINE, raw_x, box_of("got_x"), full_x, sent_x)
    conv(FINE, full_x, s["wf"].at[0], mid_f)
    step_y(1, 2)
    step_y(0, 3)
    raw_e0 = s["raw_e0"]
    conv(FINE, mid_f, s["wf"].at[1], s["e0"])

    def keep_inside(level, src, raw):
        n = level.lanes
        cells = lax.broadcasted_iota(jnp.int32, (1, n), 1)
        y, z = cells // level.stride - 2, cells % level.stride - 2
        inside = (y >= 0) & (y < level.extent) & (z >= 0) & (z < level.extent)
        for p in range(2, level.extent + 2):
            value = src[:, p * n : (p + 1) * n]
            raw[:, p * n : (p + 1) * n] = jnp.where(inside, value, jnp.zeros_like(value))

    keep_inside(FINE, s["e0"], raw_e0)

    own = raw_e0[:, 512 : 14 * 256]
    for t in range(4):
        moved = ahead(own, 16 * (t // 2) + t % 2)
        for j in range(6):
            for a in range(2):
                top = 128 * a + 32 * t
                s["cols_r"][top : top + 32, 256 * j : 256 * j + 256] = moved[
                    :, 256 * (2 * j + a) : 256 * (2 * j + a) + 256
                ]
    wide = dot(s["wr"][...], s["cols_r"][...]).astype(BF)
    rows = jnp.concatenate([wide[:, 256 * j : 256 * j + 256] for j in range(6)], axis=0)
    small = dot(rows, k["down"][...]).astype(BF)
    raw_h1 = s["raw_h1"]
    for j in range(6):
        raw_h1[:, (j + 2) * 128 : (j + 3) * 128] = small[64 * j : 64 * j + 64]
    pack(MID, raw_h1, box_of("msg_h1"))
    sent_h1 = exchange(MID, raw_h1, box_of("msg_h1"), box_of("got_h1"), s["ss"].at[1], s["rs"].at[1])
    order = [(i, d) for i in range(nzh) for d in sorted(range(ny), key=lambda d: min(d, ny - d))]
    early = [(i, d) for i, d in order if min(d, ny - d) + i < 3]

    def step_x(i, d):
        y = (gy - d + ny) % ny
        waiting["x+", i, d].wait_recv()
        j = at(zs[i], y, (gxx + nx - 1) % nx)
        if nx > 2 and i == 0:
            pass_on(j, ("f", i, d), x_next)
        pass_on(j, ("p", i, d, 1), partner)
        if nx > 2:
            waiting["x-", i, d].wait_recv()
            j = at(zs[i], y, (gxx + 1) % nx)
            if i == 1:
                pass_on(j, ("f", i, d), x_last)
            pass_on(j, ("p", i, d, 2), partner)

    step_y(1, 3)
    for i, d in early:
        step_x(i, d)
    for n in range(4, up + 1):
        step_y(0, n)
        step_y(1, n)

    full_m, mid_m = s["full_m"], s["mid_m"]
    unpack(MID, raw_h1, box_of("got_h1"), full_m, sent_h1)
    conv(MID, full_m, s["wm"].at[0], mid_m)
    conv(MID, mid_m, s["wm"].at[1], s["e1"])
    raw_e1 = s["raw_e1"]
    keep_inside(MID, s["e1"], raw_e1)

    own = raw_e1[:, 256 : 8 * 128]
    for t in range(4):
        moved = ahead(own, 10 * (t // 2) + t % 2)
        for j in range(3):
            for a in range(2):
                for ib in range(2):
                    top = 256 * ib + 128 * a + 32 * t
                    s["cols_rm"][top : top + 32, 128 * j : 128 * j + 128] = moved[
                        32 * ib : 32 * ib + 32, 128 * (2 * j + a) : 128 * (2 * j + a) + 128
                    ]
    wide = dot(s["wrm"][...], s["cols_rm"][...]).astype(BF)
    cells = dot(wide, k["down_bottom"][...]).astype(BF)
    which = group_of(64, 32)
    tile = jnp.zeros((64, 128), BF)
    for q in range(4):
        tile = jnp.where(which == q, ahead(cells[64 * q : 64 * q + 64], -32 * q), tile)
    s["msg_b"][...] = tile
    got_b = s["got_b"]
    got_b[13] = tile
    sent_b = []
    for m, (a, b, c) in enumerate(ALL26):
        slot = 9 * (a + 1) + 3 * (b + 1) + c + 1
        sent_b.append(
            send(s["msg_b"], got_b.at[slot], s["ss"].at[3, m], s["rs"].at[3, m], device(a, b, c))
        )
    pack(MID, raw_e1, box_of("msg_e1"))
    sent_e1 = exchange(MID, raw_e1, box_of("msg_e1"), box_of("got_e1"), s["ss"].at[4], s["rs"].at[4])

    for i, d in order:
        if (i, d) not in early:
            step_x(i, d)
    pack(FINE, raw_e0, box_of("msg_e0"))
    sent_e0 = exchange(FINE, raw_e0, box_of("msg_e0"), box_of("got_e0"), s["ss"].at[2], s["rs"].at[2])
    if nx > 2:
        for i, d in order:
            waiting["f", i, d].wait_recv()
            pass_on(at(zs[i], (gy - d + ny) % ny, (gxx + 2) % nx), ("p", i, d, 3), partner)

    for copy in sent_b:
        copy.wait_recv()
    for q in range(4):
        tiles = []
        for t in range(7):
            tile = jnp.zeros((64, 128), BF)
            for b in range(4):
                if 4 * t + b < 27:
                    tile = jnp.where(
                        which == b, ahead(got_b[4 * t + b], 32 * (q - b)), tile
                    )
            tiles.append(tile)
        s["b0"][64 * q : 64 * q + 64, :] = dot(jnp.concatenate(tiles, axis=1), blocks[...]).astype(BF)
    for key, copy in waiting.items():
        if key[0] == "p":
            copy.wait_recv()
    cols_b, acc = s["cols_b"], s["acc"]
    cols_b[864:896, :] = jnp.zeros((32, OUT1), BF)

    def bottom(src, m, dst, width):
        acc[:, :width] = jnp.zeros((256, width), F32)

        def one(kk, carry):
            rows = src[pl.ds(pl.multiple_of(kk * 32, 32), 32), :]
            for t in range(27):
                shift = 81 * (t // 9) + 9 * (t // 3 % 3) + t % 3
                cols_b[32 * t : 32 * t + 32, :width] = ahead(rows, shift)[:, :width]
            lhs = g_ref[m, kk % 2, pl.ds(pl.multiple_of(kk // 2 * 256, 256), 256), :]
            acc[:, :width] += dot(lhs, cols_b[:, :width])
            return carry

        lax.fori_loop(0, 8, one, 0)
        dst[...] = jnp.maximum(acc[:, :width], 0.0).astype(BF)

    bottom(s["b0"], 0, s["b1"], OUT1)
    bottom(s["b1"], 1, s["b2"], OUT2)

    full_e1 = s["full_e1"]
    unpack(MID, raw_e1, box_of("got_e1"), full_e1, sent_e1)
    base = s["b2"][...]
    for j in range(5):
        spread = dot(ahead(base, 81 * j)[:, :128], k["up_mid"][...]).astype(BF)
        rows = jnp.concatenate([spread[:, 128 * q : 128 * q + 128] for q in range(4)], axis=0)
        risen = dot(s["wxm"][...], rows)
        for a in range(2):
            lanes = slice((2 * j + a) * 128, (2 * j + a + 1) * 128)
            total = risen[64 * a : 64 * a + 64] + full_e1[:, lanes].astype(F32)
            full_m[:, lanes] = total.astype(BF)
    conv(MID, full_m, s["wm"].at[2], mid_m)
    conv(MID, mid_m, s["wm"].at[3], s["f1"])
    raw_f1 = s["raw_f1"]
    keep_inside(MID, s["f1"], raw_f1)
    pack(MID, raw_f1, box_of("msg_f1"))
    sent_f1 = exchange(MID, raw_f1, box_of("msg_f1"), box_of("got_f1"), s["ss"].at[5], s["rs"].at[5])

    full_e0 = s["full_e0"]
    unpack(FINE, raw_e0, box_of("got_e0"), full_e0, sent_e0)
    unpack(MID, raw_f1, box_of("got_f1"), s["full_f1"], sent_f1)
    for j in range(8):
        spread = dot(s["full_f1"][:, (j + 1) * 128 : (j + 2) * 128], k["up_fine"][...]).astype(BF)
        rows = jnp.concatenate([spread[:, 256 * q : 256 * q + 256] for q in range(4)], axis=0)
        risen = dot(s["wx"][...], rows)
        for a in range(2):
            lanes = slice((2 * j + a) * 256, (2 * j + a + 1) * 256)
            total = risen[32 * a : 32 * a + 32] + full_e0[:, lanes].astype(F32)
            full_x[:, lanes] = total.astype(BF)
    conv(FINE, full_x, s["wf"].at[2], mid_f)
    conv(FINE, mid_f, s["wf"].at[3], s["e0"])
    rows = jnp.concatenate([s["e0"][:, (p + 2) * 256 : (p + 3) * 256] for p in range(12)], axis=0)
    out_ref[...] = dot(rows, k["leave"][...])[:, :144].astype(BF)
    for copy in started:
        copy.wait_send()


def scratch(nyz, place_of):
    nzh, ny, nx = place_of
    fine, mid = (32, 16 * 256), (64, 10 * 128)
    count = 1 + nzh * (ny - 1) + 3 * nzh * ny + nyz
    vm = lambda *shape: pltpu.VMEM(shape, BF)
    return dict(
        raw_x=vm(*fine), full_x=vm(*fine), mid_f=vm(*fine), e0=vm(*fine), raw_e0=vm(*fine), full_e0=vm(*fine),
        raw_h1=vm(*mid), full_m=vm(*mid), mid_m=vm(*mid), e1=vm(*mid), raw_e1=vm(*mid), full_e1=vm(*mid),
        f1=vm(*mid), raw_f1=vm(*mid), full_f1=vm(*mid),
        **{
            f"{way}_{name}_{part}": vm(*shape)
            for way in ("msg", "got")
            for name in ("x", "e0", "h1", "e1", "f1")
            for part, shape in dict(
                face=(8, 3, 32, 128) if name in ("x", "e0") else (8, 1, 64, 128),
                wing=(2, 8, 16, 128),
                corner=(8, 16, 128),
                end=(2, 64, 128),
            ).items()
            if part != "end" or name not in ("x", "e0")
        },
        msg_b=vm(64, 128), got_b=vm(27, 64, 128),
        b0=vm(256, FLAT), b1=vm(256, OUT1), b2=vm(256, OUT2),
        wf=vm(4, 96, 288), wm=vm(4, 192, 576), wr=vm(64, 256), wrm=vm(256, 512), wx=vm(64, 256), wxm=vm(128, 1024),
        gathered=vm(2, 2, 1024, 896), taps=vm(864, 896), blocks=vm(FLAT, FLAT),
        cols_f=vm(288, 1024), cols_m=vm(576, 640), cols_r=vm(256, 1536), cols_rm=vm(512, 384), cols_b=vm(896, OUT1),
        sums_f=pltpu.VMEM((96, 16 * 256), F32), sums_m=pltpu.VMEM((192, 1280), F32), acc=pltpu.VMEM((256, OUT1), F32),
        ss=pltpu.SemaphoreType.DMA((6, 26)), rs=pltpu.SemaphoreType.DMA((6, 26)),
        gs=pltpu.SemaphoreType.DMA((count,)), gr=pltpu.SemaphoreType.DMA((count,)), ps=pltpu.SemaphoreType.DMA((2,)),
    )


SCRATCH = tuple(scratch(64, (2, 8, 4)))


def solution(mesh):
    ngx, nyz = mesh.shape["gx"], mesh.shape["yz"]
    place_of = (2, 8, 4) if nyz == 64 else (1, math.isqrt(nyz), math.isqrt(nyz))
    tables = {name: np.asarray(value, BF) for name, value in constants().items()}

    def body(features_in, *weights):
        planes = features_in[0].transpose(1, 0, 2).reshape(384, 144)
        result = pl.pallas_call(
            lambda *refs: kernel(ngx, nyz, place_of, *refs),
            name="unet",
            out_shape=jax.ShapeDtypeStruct((384, 144), BF),
            in_specs=[pl.BlockSpec(memory_space=pltpu.VMEM)] * (1 + len(NAMES) + len(CONST)),
            out_specs=pl.BlockSpec(memory_space=pltpu.VMEM),
            scratch_shapes=list(scratch(nyz, place_of).values()),
            compiler_params=pltpu.CompilerParams(
                collective_id=0, has_side_effects=True, vmem_limit_bytes=60 * 2**20
            ),
        )(planes, *weights, *(jnp.asarray(tables[name]) for name in CONST))
        return result.reshape(12, 32, 144).transpose(1, 0, 2)[None]

    placed = tuple(
        P("yz", None, "gx", None) if i == 0 else P("yz", None) if i in (7, 8) else P() for i in range(15)
    )
    return jax.shard_map(
        body, mesh=mesh, in_specs=placed, out_specs=P("yz", None, "gx", None), check_vma=False
    )
```
